32 devices in a mesh: dp: 1 (over z), tp: 4 (over y), pp: 8 (over x, core).
Axes of the slice: x: 4, y: 4, z: 1, core: 2. Of those that a mesh axis runs over, the one named last changes fastest.
The devices are a block of a 4x4x8 slice.
Arguments:
- tokens_in: bfloat16 [8, 128, 1024], P('dp')
- targets: bfloat16 [8, 128, 1024], P('dp')
- w_in: bfloat16 [8, 2, 1024, 4096], P('pp', None, None, 'tp')
- w_out: bfloat16 [8, 2, 4096, 1024], P('pp', None, 'tp')
Outputs:
- output 1: float32 [8, 2, 1024, 4096], P(('dp', 'pp'), None, None, 'tp')
- output 2: float32 [8, 2, 4096, 1024], P(('dp', 'pp'), None, 'tp')
- output 3: float32 [1], P('dp')
All inputs are finite; a program needn't handle non-finite values.
Results may differ from the reference program's by a relative error of at most 0.0120252.
Values are sent between devices in bfloat16 or wider.
A program may use at most 768 MiB of HBM per device.

```python
import jax
import jax.numpy as jnp
from jax import lax

STAGES = 8
MICRO = 8
TOKENS = 128
D = 1024
FF = 4096


def setup_inputs(seed: int = 0, part: int = 0) -> dict:
    base_key = jax.random.key(seed)
    shared_key, data_base = jax.random.split(base_key)
    data_key = jax.random.fold_in(data_base, part)
    x_key, y_key = jax.random.split(data_key)
    first_key, second_key = jax.random.split(shared_key)
    n_layers = 2 * STAGES
    tokens_in = jax.random.normal(x_key, (MICRO, TOKENS, D), jnp.float32).astype(jnp.bfloat16)
    targets = (1.5 * jax.random.normal(y_key, (MICRO, TOKENS, D), jnp.float32)).astype(jnp.bfloat16)
    w_in = (jax.random.normal(first_key, (STAGES, 2, D, FF), jnp.float32) * D ** -0.5).astype(jnp.bfloat16)
    w_out = (jax.random.normal(second_key, (STAGES, 2, FF, D), jnp.float32) * (2.0 * (FF * n_layers) ** -0.5)).astype(jnp.bfloat16)
    return {"tokens_in": tokens_in, "targets": targets, "w_in": w_in, "w_out": w_out}


def reference(tokens_in, targets, w_in, w_out):
    n_layers = 2 * STAGES
    stack_in = w_in.reshape(n_layers, D, FF)
    stack_out = w_out.reshape(n_layers, FF, D)
    inv_count = 1.0 / (MICRO * TOKENS * D)

    def fwd_step(act_in, weights):
        w_first, w_second = weights
        pre_act = jnp.dot(act_in, w_first, preferred_element_type=jnp.float32).astype(jnp.bfloat16)
        post_act = jax.nn.gelu(pre_act.astype(jnp.float32)).astype(jnp.bfloat16)
        branch = jnp.dot(post_act, w_second, preferred_element_type=jnp.float32)
        act_out = (act_in.astype(jnp.float32) + branch).astype(jnp.bfloat16)
        return act_out, (act_in, pre_act, post_act)

    def bwd_step(cur_grad, layer_items):
        w_first, w_second, act_in, pre_act, post_act, acc_first, acc_second = layer_items
        back_grad = jnp.dot(cur_grad, w_second.T, preferred_element_type=jnp.float32)
        gelu_pull = jax.vjp(jax.nn.gelu, pre_act.astype(jnp.float32))[1]
        gate_grad = gelu_pull(back_grad)[0].astype(jnp.bfloat16)
        spread = jnp.dot(gate_grad, w_first.T, preferred_element_type=jnp.float32)
        prev_grad = (cur_grad.astype(jnp.float32) + spread).astype(jnp.bfloat16)
        new_first = acc_first + jnp.dot(act_in.T, gate_grad, preferred_element_type=jnp.float32)
        new_second = acc_second + jnp.dot(post_act.T, cur_grad, preferred_element_type=jnp.float32)
        return prev_grad, (new_first, new_second)

    def one_micro(loop_state, micro_pair):
        acc_first, acc_second, loss_sum = loop_state
        x_mb, y_mb = micro_pair
        y_out, saved_acts = lax.scan(fwd_step, x_mb, (stack_in, stack_out))
        error_val = y_out.astype(jnp.float32) - y_mb.astype(jnp.float32)
        out_grad = (error_val * inv_count).astype(jnp.bfloat16)
        last_grad, (acc_first, acc_second) = lax.scan(bwd_step, out_grad, (stack_in, stack_out) + saved_acts + (acc_first, acc_second), reverse=True)
        return (acc_first, acc_second, loss_sum + 0.5 * jnp.sum(error_val * error_val)), None

    init_state = (jnp.zeros((n_layers, D, FF), jnp.float32), jnp.zeros((n_layers, FF, D), jnp.float32), jnp.zeros((), jnp.float32))
    (acc_first, acc_second, loss_sum), last_ys = lax.scan(one_micro, init_state, (tokens_in, targets))
    return (acc_first.reshape(STAGES, 2, D, FF), acc_second.reshape(STAGES, 2, FF, D), (loss_sum * inv_count).reshape(1))
```

```python
import functools
import math

import jax
import jax.numpy as jnp
from jax import lax
from jax.experimental import pallas as pl
from jax.experimental.pallas import tpu as pltpu
from jax.sharding import PartitionSpec as P

F32 = jnp.float32
BF16 = jnp.bfloat16
CHUNK = 128
SPACING = 3
SHIFT = 0
GELU_C = math.sqrt(2.0 / math.pi)
GELU_K = 0.044715


def gelu_fwd(u):
    return 0.5 * u * (1.0 + jnp.tanh(GELU_C * (u + GELU_K * (u * u * u))))


def gelu_grad(u):
    sq = u * u
    th = jnp.tanh(GELU_C * (u + GELU_K * (sq * u)))
    return 0.5 * (1.0 + th) + (0.5 * GELU_C) * u * (1.0 - th * th) * (1.0 + (3.0 * GELU_K) * sq)


def dot(a, b):
    return jnp.dot(a, b, preferred_element_type=F32)


def dot_t(a, b):
    return lax.dot_general(a, b, (((1,), (1,)), ((), ())), preferred_element_type=F32)


def stack_kernel(n_pp, n_tp, rows_mb, spacing, shift, inv_count,
                 x_hbm, y_hbm, w1_hbm, w2_hbm,
                 a_out, dh_out, z_out, g_out, loss_out,
                 w1, w2, a_buf, dh_buf, u_buf, z_buf, g_buf, rs_recv, rs_send, hs_send,
                 own_part, t_buf, loss_acc, loss_all, loss_tot,
                 load_sem, rs_rsem, ag_rsem, rs_ssem, ag_ssem, out_sem,
                 lall_rsem, ltot_rsem, loss_ssem):
    t = lax.axis_index("tp")
    s = lax.axis_index("pp")
    last = n_pp - 1
    n_tok = a_buf.shape[2]
    ds = a_buf.shape[3]
    hidden = w1.shape[2]
    n_mb = n_tok // rows_mb
    n_layer = 2 * n_pp
    hc = 256

    def peer(d):
        return lax.rem(t + d, n_tp)

    far_first = (2, 1, 3)

    loads = []
    for layer in range(2):
        loads.append(pltpu.make_async_copy(w1_hbm.at[layer], w1.at[layer], load_sem.at[layer]))
        for j in range(n_tp):
            loads.append(pltpu.make_async_copy(
                w2_hbm.at[layer, :, pl.ds(j * ds, ds)], w2.at[layer, j], load_sem.at[2 + layer * n_tp + j]))
    x_loads = [pltpu.make_async_copy(x_hbm.at[:, pl.ds(j * ds, ds)], a_buf.at[0, j], load_sem.at[2 + 2 * n_tp + j])
               for j in range(n_tp)]
    y_load = pltpu.make_async_copy(y_hbm.at[:, pl.ds(pl.multiple_of(t * ds, ds), ds)], t_buf, load_sem.at[2 + 3 * n_tp])

    @pl.when(s == 0)
    def _():
        for c in x_loads:
            c.start()

    for c in loads:
        c.start()

    @pl.when(s == last)
    def _():
        y_load.start()
        loss_acc[...] = jnp.zeros_like(loss_acc)

    @pl.when(s == 0)
    def _():
        for c in x_loads:
            c.wait()

    for c in loads:
        c.wait()

    @pl.when(s == last)
    def _():
        y_load.wait()

    def rows_of(m):
        return pl.ds(pl.multiple_of(m * rows_mb, rows_mb), rows_mb)

    def wait_slices(buf, layer, lp, m, with_own):
        rows = rows_of(m)
        for d in ((0,) if with_own else ()) + (1, 3, 2):
            j = peer(d)
            ref = buf.at[layer, j, rows]
            pltpu.make_async_copy(ref, ref, ag_rsem.at[lp, j, m]).wait()

    def copy_out_slices(buf, out, layer, m, sem):
        rows = rows_of(m)
        for j in range(n_tp):
            pltpu.make_async_copy(buf.at[layer, j, rows], out.at[layer, rows, pl.ds(j * ds, ds)], sem).start()

    def send_part(lp, d, m):
        rows = rows_of(m)
        pltpu.make_async_remote_copy(
            src_ref=rs_send.at[lp, d - 1, rows], dst_ref=rs_recv.at[lp, d - 1, rows],
            send_sem=rs_ssem.at[lp], recv_sem=rs_rsem.at[lp, d - 1, m],
            device_id={"pp": s, "tp": peer(d)}, device_id_type=pl.DeviceIdType.MESH).start()

    def send_slice(lp, buf, layer, lp_dst, stage, d, m):
        rows = rows_of(m)
        pltpu.make_async_remote_copy(
            src_ref=hs_send.at[lp, rows], dst_ref=buf.at[layer, t, rows],
            send_sem=ag_ssem.at[lp], recv_sem=ag_rsem.at[lp_dst, t, m],
            device_id={"pp": stage, "tp": peer(d)}, device_id_type=pl.DeviceIdType.MESH).start()

    def partials(lp, m, fn):
        rows = rows_of(m)
        for d in far_first:
            rs_send[lp, d - 1, rows, :] = fn(peer(d)).astype(BF16)
            send_part(lp, d, m)
        own_part[lp] = fn(t)

    def reduce_own(lp, m):
        rows = rows_of(m)
        for d in (1, 3, 2):
            ref = rs_recv.at[lp, d - 1, rows]
            pltpu.make_async_copy(ref, ref, rs_rsem.at[lp, d - 1, m]).wait()
        acc = own_part[lp]
        for d in (1, 3, 2):
            acc = acc + rs_recv[lp, d - 1, rows, :].astype(F32)
        return acc

    def fwd_a(layer, m):
        rows = rows_of(m)
        if layer == 0:
            @pl.when(s > 0)
            def _():
                wait_slices(a_buf, 0, 0, m, True)
        else:
            wait_slices(a_buf, 1, 1, m, False)
        for c in range(hidden // hc):
            cols = slice(c * hc, (c + 1) * hc)
            acc = dot(a_buf[layer, 0, rows, :], w1[layer, 0:ds, cols])
            for j in range(1, n_tp):
                acc = acc + dot(a_buf[layer, j, rows, :], w1[layer, j * ds:(j + 1) * ds, cols])
            u = acc.astype(BF16)
            u_buf[layer, rows, cols] = u
            z_buf[layer, rows, cols] = gelu_fwd(u.astype(F32)).astype(BF16)
        partials(layer, m, lambda j: dot(z_buf[layer, rows, :], w2[layer, j]))
        copy_out_slices(a_buf, a_out, layer, m, out_sem.at[layer])
        pltpu.make_async_copy(z_buf.at[layer, rows], z_out.at[layer, rows], out_sem.at[4 + layer]).start()

    def fwd_b(layer, m):
        rows = rows_of(m)
        acc = reduce_own(layer, m)
        h = (a_buf[layer, t, rows, :].astype(F32) + acc).astype(BF16)
        if layer == 0:
            hs_send[0, rows, :] = h
            for d in far_first:
                send_slice(0, a_buf, 1, 1, s, d, m)
            a_buf[1, t, rows, :] = h
        else:
            @pl.when(s < last)
            def _():
                hs_send[1, rows, :] = h
                for d in far_first + (0,):
                    send_slice(1, a_buf, 0, 0, s + 1, d, m)

            @pl.when(s == last)
            def _():
                err = h.astype(F32) - t_buf[rows, :].astype(F32)
                grad = (err * inv_count).astype(BF16)
                hs_send[1, rows, :] = grad
                for d in far_first:
                    send_slice(1, dh_buf, 1, 3, s, d, m)
                dh_buf[1, t, rows, :] = grad
                half = 0.5 * err * err
                half = jnp.sum(half.reshape(rows_mb // 8, 8, ds), axis=0)
                part = half[:, :128]
                for q in range(1, ds // 128):
                    part = part + half[:, q * 128:(q + 1) * 128]
                loss_acc[...] = loss_acc[...] + part

                @pl.when(m == n_mb - 1)
                def _():
                    loss_all[t] = loss_acc[...]
                    for d in far_first:
                        pltpu.make_async_remote_copy(
                            src_ref=loss_acc, dst_ref=loss_all.at[t],
                            send_sem=loss_ssem.at[0], recv_sem=lall_rsem.at[t],
                            device_id={"pp": s, "tp": peer(d)}, device_id_type=pl.DeviceIdType.MESH).start()

    def pass_loss():
        @pl.when(s == last)
        def _():
            for d in (1, 3, 2):
                j = peer(d)
                pltpu.make_async_copy(loss_all.at[j], loss_all.at[j], lall_rsem.at[j]).wait()
            tot = loss_all[0]
            for j in range(1, n_tp):
                tot = tot + loss_all[j]
            loss_tot[...] = tot

        @pl.when(s < last)
        def _():
            pltpu.make_async_copy(loss_tot, loss_tot, ltot_rsem).wait()

        @pl.when(s > 0)
        def _():
            pltpu.make_async_remote_copy(
                src_ref=loss_tot, dst_ref=loss_tot, send_sem=loss_ssem.at[1], recv_sem=ltot_rsem,
                device_id={"pp": s - 1, "tp": t}, device_id_type=pl.DeviceIdType.MESH).start()

    def bwd_a(layer, m):
        lp = 2 + layer
        rows = rows_of(m)
        if layer == 1:
            @pl.when(s < last)
            def _():
                wait_slices(dh_buf, 1, 3, m, True)

            @pl.when(s == last)
            def _():
                wait_slices(dh_buf, 1, 3, m, False)
        else:
            wait_slices(dh_buf, 0, 2, m, False)
        for c in range(hidden // hc):
            cols = slice(c * hc, (c + 1) * hc)
            acc = dot_t(dh_buf[layer, 0, rows, :], w2[layer, 0, cols, :])
            for j in range(1, n_tp):
                acc = acc + dot_t(dh_buf[layer, j, rows, :], w2[layer, j, cols, :])
            u = u_buf[layer, rows, cols].astype(F32)
            g_buf[layer, rows, cols] = (gelu_grad(u) * acc).astype(BF16)

        def send():
            partials(lp, m, lambda j: dot_t(
                g_buf[layer, rows, :], w1[layer, pl.ds(pl.multiple_of(j * ds, ds), ds), :]))

        if layer == 1:
            send()
        else:
            pl.when(s > 0)(send)
        copy_out_slices(dh_buf, dh_out, layer, m, out_sem.at[2 + layer])
        pltpu.make_async_copy(g_buf.at[layer, rows], g_out.at[layer, rows], out_sem.at[6 + layer]).start()
        if layer == 1:
            pl.when(m == n_mb - 1)(pass_loss)

    def bwd_b(layer, m):
        lp = 2 + layer
        rows = rows_of(m)
        acc = reduce_own(lp, m)
        h = (dh_buf[layer, t, rows, :].astype(F32) + acc).astype(BF16)
        hs_send[lp, rows, :] = h
        if layer == 1:
            for d in far_first:
                send_slice(lp, dh_buf, 0, 2, s, d, m)
            dh_buf[0, t, rows, :] = h
        else:
            for d in far_first + (0,):
                send_slice(lp, dh_buf, 1, 3, s - 1, d, m)

    def at_tick(k, start, fn, layer, extra=None):
        q = k - start
        m = lax.div(q, spacing)
        ok = (q >= 0) & (lax.rem(q, spacing) == 0) & (m < n_mb)
        if extra is not None:
            ok = ok & extra
        pl.when(ok)(lambda: fn(layer, m))

    f_start = 4 * s
    b_start = 2 * n_layer + shift + 4 * (last - s)

    def tick(k, carry):
        at_tick(k, f_start + 1, fwd_b, 0)
        at_tick(k, f_start + 3, fwd_b, 1)
        at_tick(k, b_start + 1, bwd_b, 1)
        at_tick(k, b_start + 3, bwd_b, 0, s > 0)
        at_tick(k, b_start, bwd_a, 1)
        at_tick(k, b_start + 2, bwd_a, 0)
        at_tick(k, f_start, fwd_a, 0)
        at_tick(k, f_start + 2, fwd_a, 1)
        return carry

    n_ticks = 4 * n_layer + shift + spacing * (n_mb - 1)
    lax.fori_loop(0, n_ticks, tick, 0)

    for layer in range(2):
        for i in range(4):
            pltpu.make_async_copy(z_buf.at[layer], z_out.at[layer], out_sem.at[2 * i + layer]).wait()

    def wait_three(sem):
        pltpu.make_async_copy(rs_send.at[0], rs_send.at[0], sem).wait()

    def wait_four(sem):
        pltpu.make_async_copy(a_buf.at[0], a_buf.at[0], sem).wait()

    for lp in (0, 1, 3):
        wait_three(rs_ssem.at[lp])
    wait_three(ag_ssem.at[0])
    wait_three(ag_ssem.at[3])

    @pl.when(s < last)
    def _():
        wait_four(ag_ssem.at[1])

    @pl.when(s == last)
    def _():
        wait_three(ag_ssem.at[1])
        pltpu.make_async_copy(loss_all.at[0:3], loss_all.at[0:3], loss_ssem.at[0]).wait()

    @pl.when(s > 0)
    def _():
        wait_three(rs_ssem.at[2])
        wait_four(ag_ssem.at[2])
        pltpu.make_async_copy(loss_tot, loss_tot, loss_ssem.at[1]).wait()

    loss_out[...] = loss_tot[...]


def solution(mesh):
    n_pp = mesh.shape["pp"]
    n_tp = mesh.shape["tp"]

    def device_program(x_loc, y_loc, w_in, w_out):
        n_tok = x_loc.shape[0] * x_loc.shape[1]
        d_model = x_loc.shape[2]
        hidden = w_in.shape[3]
        ds = d_model // n_tp
        rows_mb = CHUNK
        n_mb = n_tok // rows_mb
        inv_count = 1.0 / (n_tok * d_model)
        kernel = functools.partial(stack_kernel, n_pp, n_tp, rows_mb, SPACING, SHIFT, inv_count)
        any_spec = pl.BlockSpec(memory_space=pl.ANY)
        dma = pltpu.SemaphoreType.DMA
        a, dh, z, g, loss = pl.pallas_call(
            kernel,
            out_shape=[
                jax.ShapeDtypeStruct((2, n_tok, d_model), BF16),
                jax.ShapeDtypeStruct((2, n_tok, d_model), BF16),
                jax.ShapeDtypeStruct((2, n_tok, hidden), BF16),
                jax.ShapeDtypeStruct((2, n_tok, hidden), BF16),
                jax.ShapeDtypeStruct((8, 128), F32),
            ],
            in_specs=[any_spec] * 4,
            out_specs=[any_spec] * 4 + [pl.BlockSpec(memory_space=pltpu.VMEM)],
            scratch_shapes=[
                pltpu.VMEM((2, d_model, hidden), BF16),
                pltpu.VMEM((2, n_tp, hidden, ds), BF16),
                pltpu.VMEM((2, n_tp, n_tok, ds), BF16),
                pltpu.VMEM((2, n_tp, n_tok, ds), BF16),
                pltpu.VMEM((2, n_tok, hidden), BF16),
                pltpu.VMEM((2, n_tok, hidden), BF16),
                pltpu.VMEM((2, n_tok, hidden), BF16),
                pltpu.VMEM((4, 3, n_tok, ds), BF16),
                pltpu.VMEM((4, 3, n_tok, ds), BF16),
                pltpu.VMEM((4, n_tok, ds), BF16),
                pltpu.VMEM((4, rows_mb, ds), F32),
                pltpu.VMEM((n_tok, ds), BF16),
                pltpu.VMEM((8, 128), F32),
                pltpu.VMEM((n_tp, 8, 128), F32),
                pltpu.VMEM((8, 128), F32),
                dma((3 + 3 * n_tp,)),
                dma((4, 3, n_mb)),
                dma((4, n_tp, n_mb)),
                dma((4,)),
                dma((4,)),
                dma((8,)),
                dma((n_tp,)),
                dma,
                dma((2,)),
            ],
            compiler_params=pltpu.CompilerParams(has_side_effects=True, vmem_limit_bytes=60 * 1024 * 1024),
            cost_estimate=pl.CostEstimate(flops=10**11, bytes_accessed=10**8, transcendentals=0),
            name="mlp_stack",
        )(x_loc.reshape(n_tok, d_model), y_loc.reshape(n_tok, d_model), w_in[0], w_out[0])
        grad_first = jnp.einsum("ltd,ltf->ldf", a, g, preferred_element_type=F32)[None]
        grad_second = jnp.einsum("ltf,ltd->lfd", z, dh, preferred_element_type=F32)[None]
        loss_val = (jnp.sum(loss) * inv_count).reshape(1)
        return grad_first, grad_second, loss_val

    return jax.shard_map(
        device_program,
        mesh=mesh,
        in_specs=(P("dp", None, None), P("dp", None, None), P("pp", None, None, "tp"), P("pp", None, "tp", None)),
        out_specs=(P(("dp", "pp"), None, None, "tp"), P(("dp", "pp"), None, "tp", None), P("dp")),
        check_vma=False,
    )
```

```python
import functools
import math

import jax
import jax.numpy as jnp
from jax import lax
from jax.experimental import pallas as pl
from jax.experimental.pallas import tpu as pltpu
from jax.sharding import PartitionSpec as P

F32 = jnp.float32
BF16 = jnp.bfloat16
CHUNK = 64
SPACING = 1
SHIFT = 0
GELU_C = math.sqrt(2.0 / math.pi)
GELU_K = 0.044715


def gelu_fwd(u):
    return 0.5 * u * (1.0 + jnp.tanh(GELU_C * (u + GELU_K * (u * u * u))))


def gelu_grad(u):
    sq = u * u
    th = jnp.tanh(GELU_C * (u + GELU_K * (sq * u)))
    return 0.5 * (1.0 + th) + (0.5 * GELU_C) * u * (1.0 - th * th) * (1.0 + (3.0 * GELU_K) * sq)


def dot(a, b):
    return jnp.dot(a, b, preferred_element_type=F32)


def dot_t(a, b):
    return lax.dot_general(a, b, (((1,), (1,)), ((), ())), preferred_element_type=F32)


def stack_kernel(n_pp, n_tp, rows_mb, spacing, shift, inv_count,
                 x_hbm, y_hbm, w1_hbm, w2_hbm,
                 a_out, dh_out, z_out, g_out, loss_out,
                 w1, w2, a_buf, dh_buf, u_buf, z_buf, g_buf, rs_recv, rs_send, hs_send,
                 own_part, t_buf, loss_acc, loss_all, loss_tot,
                 load_sem, rs_rsem, ag_rsem, rs_ssem, ag_ssem, out_sem,
                 lall_rsem, ltot_rsem, loss_ssem):
    t = lax.axis_index("tp")
    s = lax.axis_index("pp")
    last = n_pp - 1
    n_tok = a_buf.shape[2]
    ds = a_buf.shape[3]
    hidden = w1.shape[2]
    n_mb = n_tok // rows_mb
    n_layer = 2 * n_pp
    hc = 256

    def peer(d):
        return lax.rem(t + d, n_tp)

    far_first = (2, 1, 3)

    loads = []
    for layer in range(2):
        loads.append(pltpu.make_async_copy(w1_hbm.at[layer], w1.at[layer], load_sem.at[layer]))
        for j in range(n_tp):
            loads.append(pltpu.make_async_copy(
                w2_hbm.at[layer, :, pl.ds(j * ds, ds)], w2.at[layer, j], load_sem.at[2 + layer * n_tp + j]))
    x_loads = [pltpu.make_async_copy(x_hbm.at[:, pl.ds(j * ds, ds)], a_buf.at[0, j], load_sem.at[2 + 2 * n_tp + j])
               for j in range(n_tp)]
    y_load = pltpu.make_async_copy(y_hbm.at[:, pl.ds(pl.multiple_of(t * ds, ds), ds)], t_buf, load_sem.at[2 + 3 * n_tp])

    @pl.when(s == 0)
    def _():
        for c in x_loads:
            c.start()

    for c in loads:
        c.start()

    @pl.when(s == last)
    def _():
        y_load.start()
        loss_acc[...] = jnp.zeros_like(loss_acc)

    @pl.when(s == 0)
    def _():
        for c in x_loads:
            c.wait()

    for c in loads:
        c.wait()

    @pl.when(s == last)
    def _():
        y_load.wait()

    def rows_of(m):
        return pl.ds(pl.multiple_of(m * rows_mb, rows_mb), rows_mb)

    def wait_slices(buf, layer, lp, m, with_own):
        rows = rows_of(m)
        for d in ((0,) if with_own else ()) + (1, 3, 2):
            j = peer(d)
            ref = buf.at[layer, j, rows]
            pltpu.make_async_copy(ref, ref, ag_rsem.at[lp, j, m]).wait()

    def copy_out_slices(buf, out, layer, m, sem):
        rows = rows_of(m)
        for j in range(n_tp):
            pltpu.make_async_copy(buf.at[layer, j, rows], out.at[layer, rows, pl.ds(j * ds, ds)], sem).start()

    def send_part(lp, d, m):
        rows = rows_of(m)
        pltpu.make_async_remote_copy(
            src_ref=rs_send.at[lp, d - 1, rows], dst_ref=rs_recv.at[lp, d - 1, rows],
            send_sem=rs_ssem.at[lp], recv_sem=rs_rsem.at[lp, d - 1, m],
            device_id={"pp": s, "tp": peer(d)}, device_id_type=pl.DeviceIdType.MESH).start()

    def send_slice(lp, buf, layer, lp_dst, stage, d, m):
        rows = rows_of(m)
        pltpu.make_async_remote_copy(
            src_ref=hs_send.at[lp, rows], dst_ref=buf.at[layer, t, rows],
            send_sem=ag_ssem.at[lp], recv_sem=ag_rsem.at[lp_dst, t, m],
            device_id={"pp": stage, "tp": peer(d)}, device_id_type=pl.DeviceIdType.MESH).start()

    def partials(lp, m, fn):
        rows = rows_of(m)
        for d in far_first:
            rs_send[lp, d - 1, rows, :] = fn(peer(d)).astype(BF16)
            send_part(lp, d, m)
        own_part[lp] = fn(t)

    def reduce_own(lp, m):
        rows = rows_of(m)
        for d in (1, 3, 2):
            ref = rs_recv.at[lp, d - 1, rows]
            pltpu.make_async_copy(ref, ref, rs_rsem.at[lp, d - 1, m]).wait()
        acc = own_part[lp]
        for d in (1, 3, 2):
            acc = acc + rs_recv[lp, d - 1, rows, :].astype(F32)
        return acc

    def fwd_a(layer, m):
        rows = rows_of(m)
        if layer == 0:
            @pl.when(s > 0)
            def _():
                wait_slices(a_buf, 0, 0, m, True)
        else:
            wait_slices(a_buf, 1, 1, m, False)
        for c in range(hidden // hc):
            cols = slice(c * hc, (c + 1) * hc)
            acc = dot(a_buf[layer, 0, rows, :], w1[layer, 0:ds, cols])
            for j in range(1, n_tp):
                acc = acc + dot(a_buf[layer, j, rows, :], w1[layer, j * ds:(j + 1) * ds, cols])
            u = acc.astype(BF16)
            u_buf[layer, rows, cols] = u
            z_buf[layer, rows, cols] = gelu_fwd(u.astype(F32)).astype(BF16)
        partials(layer, m, lambda j: dot(z_buf[layer, rows, :], w2[layer, j]))
        copy_out_slices(a_buf, a_out, layer, m, out_sem.at[layer])
        pltpu.make_async_copy(z_buf.at[layer, rows], z_out.at[layer, rows], out_sem.at[4 + layer]).start()

    def fwd_b(layer, m):
        rows = rows_of(m)
        acc = reduce_own(layer, m)
        h = (a_buf[layer, t, rows, :].astype(F32) + acc).astype(BF16)
        if layer == 0:
            hs_send[0, rows, :] = h
            for d in far_first:
                send_slice(0, a_buf, 1, 1, s, d, m)
            a_buf[1, t, rows, :] = h
        else:
            @pl.when(s < last)
            def _():
                hs_send[1, rows, :] = h
                for d in far_first + (0,):
                    send_slice(1, a_buf, 0, 0, s + 1, d, m)

            @pl.when(s == last)
            def _():
                err = h.astype(F32) - t_buf[rows, :].astype(F32)
                grad = (err * inv_count).astype(BF16)
                hs_send[1, rows, :] = grad
                for d in far_first:
                    send_slice(1, dh_buf, 1, 3, s, d, m)
                dh_buf[1, t, rows, :] = grad
                half = 0.5 * err * err
                half = jnp.sum(half.reshape(rows_mb // 8, 8, ds), axis=0)
                part = half[:, :128]
                for q in range(1, ds // 128):
                    part = part + half[:, q * 128:(q + 1) * 128]
                loss_acc[...] = loss_acc[...] + part

                @pl.when(m == n_mb - 1)
                def _():
                    loss_all[t] = loss_acc[...]
                    for d in far_first:
                        pltpu.make_async_remote_copy(
                            src_ref=loss_acc, dst_ref=loss_all.at[t],
                            send_sem=loss_ssem.at[0], recv_sem=lall_rsem.at[t],
                            device_id={"pp": s, "tp": peer(d)}, device_id_type=pl.DeviceIdType.MESH).start()

    def pass_loss():
        @pl.when(s == last)
        def _():
            for d in (1, 3, 2):
                j = peer(d)
                pltpu.make_async_copy(loss_all.at[j], loss_all.at[j], lall_rsem.at[j]).wait()
            tot = loss_all[0]
            for j in range(1, n_tp):
                tot = tot + loss_all[j]
            loss_tot[...] = tot

        @pl.when(s < last)
        def _():
            pltpu.make_async_copy(loss_tot, loss_tot, ltot_rsem).wait()

        @pl.when(s > 0)
        def _():
            pltpu.make_async_remote_copy(
                src_ref=loss_tot, dst_ref=loss_tot, send_sem=loss_ssem.at[1], recv_sem=ltot_rsem,
                device_id={"pp": s - 1, "tp": t}, device_id_type=pl.DeviceIdType.MESH).start()

    def bwd_a(layer, m):
        lp = 2 + layer
        rows = rows_of(m)
        if layer == 1:
            @pl.when(s < last)
            def _():
                wait_slices(dh_buf, 1, 3, m, True)

            @pl.when(s == last)
            def _():
                wait_slices(dh_buf, 1, 3, m, False)
        else:
            wait_slices(dh_buf, 0, 2, m, False)
        for c in range(hidden // hc):
            cols = slice(c * hc, (c + 1) * hc)
            acc = dot_t(dh_buf[layer, 0, rows, :], w2[layer, 0, cols, :])
            for j in range(1, n_tp):
                acc = acc + dot_t(dh_buf[layer, j, rows, :], w2[layer, j, cols, :])
            u = u_buf[layer, rows, cols].astype(F32)
            g_buf[layer, rows, cols] = (gelu_grad(u) * acc).astype(BF16)

        def send():
            partials(lp, m, lambda j: dot_t(
                g_buf[layer, rows, :], w1[layer, pl.ds(pl.multiple_of(j * ds, ds), ds), :]))

        if layer == 1:
            send()
        else:
            pl.when(s > 0)(send)
        copy_out_slices(dh_buf, dh_out, layer, m, out_sem.at[2 + layer])
        pltpu.make_async_copy(g_buf.at[layer, rows], g_out.at[layer, rows], out_sem.at[6 + layer]).start()
        if layer == 1:
            pl.when(m == n_mb - 1)(pass_loss)

    def bwd_b(layer, m):
        lp = 2 + layer
        rows = rows_of(m)
        acc = reduce_own(lp, m)
        h = (dh_buf[layer, t, rows, :].astype(F32) + acc).astype(BF16)
        hs_send[lp, rows, :] = h
        if layer == 1:
            for d in far_first:
                send_slice(lp, dh_buf, 0, 2, s, d, m)
            dh_buf[0, t, rows, :] = h
        else:
            for d in far_first + (0,):
                send_slice(lp, dh_buf, 1, 3, s - 1, d, m)

    f_start = 4 * s
    b_start = 2 * n_layer + shift + 4 * (last - s)

    def tick(k, carry):
        bias = 8 * n_pp + 2 * n_layer + shift + 4
        bias = spacing * (-(-bias // spacing))
        turn = {}
        for name, start in (("f", f_start), ("b", b_start)):
            q = k - start + bias
            turn[name] = (lax.div(q, spacing) - bias // spacing, lax.rem(q, spacing) if spacing > 1 else None)

        def at(name, offset, fn, layer, extra=None):
            m, phase = turn[name]
            m = m - offset // spacing
            ok = (m >= 0) & (m < n_mb)
            if phase is not None:
                ok = ok & (phase == offset % spacing)
            if extra is not None:
                ok = ok & extra
            pl.when(ok)(lambda: fn(layer, m))

        at("b", 3, bwd_b, 0, s > 0)
        at("b", 2, bwd_a, 0)
        at("b", 1, bwd_b, 1)
        at("b", 0, bwd_a, 1)
        at("f", 3, fwd_b, 1)
        at("f", 2, fwd_a, 1)
        at("f", 1, fwd_b, 0)
        at("f", 0, fwd_a, 0)
        return carry

    n_ticks = 4 * n_layer + shift + spacing * (n_mb - 1)
    lax.fori_loop(0, n_ticks, tick, 0)

    for layer in range(2):
        for i in range(4):
            pltpu.make_async_copy(z_buf.at[layer], z_out.at[layer], out_sem.at[2 * i + layer]).wait()

    def wait_three(sem):
        pltpu.make_async_copy(rs_send.at[0], rs_send.at[0], sem).wait()

    def wait_four(sem):
        pltpu.make_async_copy(a_buf.at[0], a_buf.at[0], sem).wait()

    for lp in (0, 1, 3):
        wait_three(rs_ssem.at[lp])
    wait_three(ag_ssem.at[0])
    wait_three(ag_ssem.at[3])

    @pl.when(s < last)
    def _():
        wait_four(ag_ssem.at[1])

    @pl.when(s == last)
    def _():
        wait_three(ag_ssem.at[1])
        pltpu.make_async_copy(loss_all.at[0:3], loss_all.at[0:3], loss_ssem.at[0]).wait()

    @pl.when(s > 0)
    def _():
        wait_three(rs_ssem.at[2])
        wait_four(ag_ssem.at[2])
        pltpu.make_async_copy(loss_tot, loss_tot, loss_ssem.at[1]).wait()

    loss_out[...] = loss_tot[...]


def solution(mesh):
    n_pp = mesh.shape["pp"]
    n_tp = mesh.shape["tp"]

    def device_program(x_loc, y_loc, w_in, w_out):
        n_tok = x_loc.shape[0] * x_loc.shape[1]
        d_model = x_loc.shape[2]
        hidden = w_in.shape[3]
        ds = d_model // n_tp
        rows_mb = CHUNK
        n_mb = n_tok // rows_mb
        inv_count = 1.0 / (n_tok * d_model)
        kernel = functools.partial(stack_kernel, n_pp, n_tp, rows_mb, SPACING, SHIFT, inv_count)
        any_spec = pl.BlockSpec(memory_space=pl.ANY)
        dma = pltpu.SemaphoreType.DMA
        a, dh, z, g, loss = pl.pallas_call(
            kernel,
            out_shape=[
                jax.ShapeDtypeStruct((2, n_tok, d_model), BF16),
                jax.ShapeDtypeStruct((2, n_tok, d_model), BF16),
                jax.ShapeDtypeStruct((2, n_tok, hidden), BF16),
                jax.ShapeDtypeStruct((2, n_tok, hidden), BF16),
                jax.ShapeDtypeStruct((8, 128), F32),
            ],
            in_specs=[any_spec] * 4,
            out_specs=[any_spec] * 4 + [pl.BlockSpec(memory_space=pltpu.VMEM)],
            scratch_shapes=[
                pltpu.VMEM((2, d_model, hidden), BF16),
                pltpu.VMEM((2, n_tp, hidden, ds), BF16),
                pltpu.VMEM((2, n_tp, n_tok, ds), BF16),
                pltpu.VMEM((2, n_tp, n_tok, ds), BF16),
                pltpu.VMEM((2, n_tok, hidden), BF16),
                pltpu.VMEM((2, n_tok, hidden), BF16),
                pltpu.VMEM((2, n_tok, hidden), BF16),
                pltpu.VMEM((4, 3, n_tok, ds), BF16),
                pltpu.VMEM((4, 3, n_tok, ds), BF16),
                pltpu.VMEM((4, n_tok, ds), BF16),
                pltpu.VMEM((4, rows_mb, ds), F32),
                pltpu.VMEM((n_tok, ds), BF16),
                pltpu.VMEM((8, 128), F32),
                pltpu.VMEM((n_tp, 8, 128), F32),
                pltpu.VMEM((8, 128), F32),
                dma((3 + 3 * n_tp,)),
                dma((4, 3, n_mb)),
                dma((4, n_tp, n_mb)),
                dma((4,)),
                dma((4,)),
                dma((8,)),
                dma((n_tp,)),
                dma,
                dma((2,)),
            ],
            compiler_params=pltpu.CompilerParams(has_side_effects=True, vmem_limit_bytes=60 * 1024 * 1024),
            cost_estimate=pl.CostEstimate(flops=10**11, bytes_accessed=10**8, transcendentals=0),
            name="mlp_stack",
        )(x_loc.reshape(n_tok, d_model), y_loc.reshape(n_tok, d_model), w_in[0], w_out[0])
        grad_first = jnp.einsum("ltd,ltf->ldf", a, g, preferred_element_type=F32)[None]
        grad_second = jnp.einsum("ltf,ltd->lfd", z, dh, preferred_element_type=F32)[None]
        loss_val = (jnp.sum(loss) * inv_count).reshape(1)
        return grad_first, grad_second, loss_val

    return jax.shard_map(
        device_program,
        mesh=mesh,
        in_specs=(P("dp", None, None), P("dp", None, None), P("pp", None, None, "tp"), P("pp", None, "tp", None)),
        out_specs=(P(("dp", "pp"), None, None, "tp"), P(("dp", "pp"), None, "tp", None), P("dp")),
        check_vma=False,
    )
```

```python
import functools
import math

import jax
import jax.numpy as jnp
from jax import lax
from jax.experimental import pallas as pl
from jax.experimental.pallas import tpu as pltpu
from jax.sharding import PartitionSpec as P

F32 = jnp.float32
BF16 = jnp.bfloat16
CHUNK = 64
SPACING = 1
HOST = 1
GRAD_TILE = 512
SHIFT = 0
GELU_C = math.sqrt(2.0 / math.pi)
GELU_K = 0.044715


def gelu_fwd(u):
    return 0.5 * u * (1.0 + jnp.tanh(GELU_C * (u + GELU_K * (u * u * u))))


def gelu_grad(u):
    sq = u * u
    th = jnp.tanh(GELU_C * (u + GELU_K * (sq * u)))
    return 0.5 * (1.0 + th) + (0.5 * GELU_C) * u * (1.0 - th * th) * (1.0 + (3.0 * GELU_K) * sq)


def dot(a, b):
    return jnp.dot(a, b, preferred_element_type=F32)


def dot_t(a, b):
    return lax.dot_general(a, b, (((1,), (1,)), ((), ())), preferred_element_type=F32)


def stack_kernel(n_pp, n_tp, rows_mb, spacing, shift, inv_count,
                 x_hbm, y_hbm, w1_hbm, w2_hbm,
                 a_out, dh_out, z_out, g_out, loss_out,
                 w1, w2, a_buf, dh_buf, u_buf, z_buf, g_buf, rs_recv, rs_send, hs_send,
                 own_part, t_buf, loss_acc, loss_all, loss_tot,
                 guest_recv, guest_own, own_send, guest_send,
                 load_sem, rs_rsem, ag_rsem, rs_ssem, ag_ssem, out_sem,
                 guest_rsem, guest_ssem, own_ssem,
                 lall_rsem, ltot_rsem, loss_ssem):
    t = lax.axis_index("tp")
    s = lax.axis_index("pp")
    last = n_pp - 1
    away = last
    host_stage = HOST
    n_tok = a_buf.shape[2]
    ds = a_buf.shape[3]
    hidden = w1.shape[2]
    n_mb = n_tok // rows_mb
    n_layer = 2 * n_pp
    hc = 256

    def peer(d):
        return lax.rem(t + d, n_tp)

    far_first = (2, 1, 3)

    loads = [[], []]
    for layer in range(2):
        loads[layer].append(pltpu.make_async_copy(w1_hbm.at[layer], w1.at[layer], load_sem.at[layer]))
        for j in range(n_tp):
            loads[layer].append(pltpu.make_async_copy(
                w2_hbm.at[layer, :, pl.ds(j * ds, ds)], w2.at[layer, j], load_sem.at[2 + layer * n_tp + j]))
    x_loads = [pltpu.make_async_copy(x_hbm.at[:, pl.ds(j * ds, ds)], a_buf.at[0, j], load_sem.at[2 + 2 * n_tp + j])
               for j in range(n_tp)]
    y_load = pltpu.make_async_copy(y_hbm.at[:, pl.ds(pl.multiple_of(t * ds, ds), ds)], t_buf, load_sem.at[2 + 3 * n_tp])

    @pl.when(s == 0)
    def _():
        for c in x_loads:
            c.start()

    for c in loads[0] + loads[1]:
        c.start()

    @pl.when(s == host_stage)
    def _():
        y_load.start()
        loss_acc[...] = jnp.zeros_like(loss_acc)

    @pl.when(s == 0)
    def _():
        for c in x_loads:
            c.wait()

    for c in loads[0]:
        c.wait()

    @pl.when(s == host_stage)
    def _():
        y_load.wait()

    def rows_of(m):
        return pl.ds(pl.multiple_of(m * rows_mb, rows_mb), rows_mb)

    def wait_slices(buf, layer, lp, m, with_own):
        rows = rows_of(m)
        for d in ((0,) if with_own else ()) + (1, 3, 2):
            j = peer(d)
            ref = buf.at[layer, j, rows]
            pltpu.make_async_copy(ref, ref, ag_rsem.at[lp, j, m]).wait()

    def copy_out_slices(buf, out, layer, m, sem):
        rows = rows_of(m)
        for j in range(n_tp):
            pltpu.make_async_copy(buf.at[layer, j, rows], out.at[layer, rows, pl.ds(j * ds, ds)], sem).start()

    def send_part(lp, d, m):
        rows = rows_of(m)

        @pl.when(s < away)
        def _():
            pltpu.make_async_remote_copy(
                src_ref=rs_send.at[lp, d - 1, rows], dst_ref=rs_recv.at[lp, d - 1, rows],
                send_sem=rs_ssem.at[lp], recv_sem=rs_rsem.at[lp, d - 1, m],
                device_id={"pp": s, "tp": peer(d)}, device_id_type=pl.DeviceIdType.MESH).start()

        @pl.when(s >= away)
        def _():
            pltpu.make_async_remote_copy(
                src_ref=rs_send.at[lp, d - 1, rows], dst_ref=guest_recv.at[lp, d - 1, rows],
                send_sem=rs_ssem.at[lp], recv_sem=guest_rsem.at[lp, d - 1, m],
                device_id={"pp": host_stage, "tp": peer(d)}, device_id_type=pl.DeviceIdType.MESH).start()

    def send_slice(lp, buf, layer, lp_dst, stage, d, m):
        rows = rows_of(m)
        pltpu.make_async_remote_copy(
            src_ref=hs_send.at[lp, rows], dst_ref=buf.at[layer, t, rows],
            send_sem=ag_ssem.at[lp], recv_sem=ag_rsem.at[lp_dst, t, m],
            device_id={"pp": stage, "tp": peer(d)}, device_id_type=pl.DeviceIdType.MESH).start()

    def send_guest(lp, buf, layer, lp_dst, stage, m):
        rows = rows_of(m)
        for d in far_first + (0,):
            pltpu.make_async_remote_copy(
                src_ref=guest_send.at[lp, rows], dst_ref=buf.at[layer, t, rows],
                send_sem=guest_ssem.at[lp], recv_sem=ag_rsem.at[lp_dst, t, m],
                device_id={"pp": stage, "tp": peer(d)}, device_id_type=pl.DeviceIdType.MESH).start()

    def partials(lp, m, buf, layer, fn):
        rows = rows_of(m)
        for d in far_first:
            rs_send[lp, d - 1, rows, :] = fn(peer(d)).astype(BF16)
            send_part(lp, d, m)
        own = buf[layer, t, rows, :].astype(F32) + fn(t)

        @pl.when(s < away)
        def _():
            own_part[lp] = own

        @pl.when(s >= away)
        def _():
            own_send[lp, rows, :] = own
            pltpu.make_async_remote_copy(
                src_ref=own_send.at[lp, rows], dst_ref=guest_own.at[lp, rows],
                send_sem=own_ssem.at[lp], recv_sem=guest_rsem.at[lp, 3, m],
                device_id={"pp": host_stage, "tp": t}, device_id_type=pl.DeviceIdType.MESH).start()

    def reduce_own(lp, m):
        rows = rows_of(m)
        for d in (1, 3, 2):
            ref = rs_recv.at[lp, d - 1, rows]
            pltpu.make_async_copy(ref, ref, rs_rsem.at[lp, d - 1, m]).wait()
        acc = own_part[lp]
        for d in (1, 3, 2):
            acc = acc + rs_recv[lp, d - 1, rows, :].astype(F32)
        return acc.astype(BF16)

    def reduce_guest(lp, m):
        rows = rows_of(m)
        for d in (1, 3, 2):
            ref = guest_recv.at[lp, d - 1, rows]
            pltpu.make_async_copy(ref, ref, guest_rsem.at[lp, d - 1, m]).wait()
        ref = guest_own.at[lp, rows]
        pltpu.make_async_copy(ref, ref, guest_rsem.at[lp, 3, m]).wait()
        acc = guest_own[lp, rows, :]
        for d in (1, 3, 2):
            acc = acc + guest_recv[lp, d - 1, rows, :].astype(F32)
        return acc.astype(BF16)

    def fwd_a(layer, m):
        rows = rows_of(m)
        if layer == 0:
            @pl.when(s > 0)
            def _():
                wait_slices(a_buf, 0, 0, m, True)
        else:
            @pl.when(s < away)
            def _():
                wait_slices(a_buf, 1, 1, m, False)

            @pl.when(s >= away)
            def _():
                wait_slices(a_buf, 1, 1, m, True)
        for c in range(hidden // hc):
            cols = slice(c * hc, (c + 1) * hc)
            acc = dot(a_buf[layer, 0, rows, :], w1[layer, 0:ds, cols])
            for j in range(1, n_tp):
                acc = acc + dot(a_buf[layer, j, rows, :], w1[layer, j * ds:(j + 1) * ds, cols])
            u = acc.astype(BF16)
            u_buf[layer, rows, cols] = u
            z_buf[layer, rows, cols] = gelu_fwd(u.astype(F32)).astype(BF16)
        partials(layer, m, a_buf, layer, lambda j: dot(z_buf[layer, rows, :], w2[layer, j]))
        copy_out_slices(a_buf, a_out, layer, m, out_sem.at[layer])
        pltpu.make_async_copy(z_buf.at[layer, rows], z_out.at[layer, rows], out_sem.at[4 + layer]).start()

    def fwd_b(layer, m):
        rows = rows_of(m)
        h = reduce_own(layer, m)
        hs_send[layer, rows, :] = h
        if layer == 0:
            for d in far_first:
                send_slice(0, a_buf, 1, 1, s, d, m)
            a_buf[1, t, rows, :] = h
        else:
            for d in far_first + (0,):
                send_slice(1, a_buf, 0, 0, s + 1, d, m)

    def fwd_b_guest(layer, m):
        rows = rows_of(m)
        h = reduce_guest(layer, m)
        if layer == 0:
            guest_send[0, rows, :] = h
            send_guest(0, a_buf, 1, 1, last, m)
            return
        err = h.astype(F32) - t_buf[rows, :].astype(F32)
        guest_send[1, rows, :] = (err * inv_count).astype(BF16)
        send_guest(1, dh_buf, 1, 3, last, m)
        half = 0.5 * err * err
        half = jnp.sum(half.reshape(rows_mb // 8, 8, ds), axis=0)
        part = half[:, :128]
        for q in range(1, ds // 128):
            part = part + half[:, q * 128:(q + 1) * 128]
        loss_acc[...] = loss_acc[...] + part

        @pl.when(m == n_mb - 1)
        def _():
            for d in far_first + (0,):
                pltpu.make_async_remote_copy(
                    src_ref=loss_acc, dst_ref=loss_all.at[t],
                    send_sem=loss_ssem.at[0], recv_sem=lall_rsem.at[t],
                    device_id={"pp": last, "tp": peer(d)}, device_id_type=pl.DeviceIdType.MESH).start()

    def pass_loss():
        @pl.when(s == last)
        def _():
            for j in range(n_tp):
                pltpu.make_async_copy(loss_all.at[j], loss_all.at[j], lall_rsem.at[j]).wait()
            tot = loss_all[0]
            for j in range(1, n_tp):
                tot = tot + loss_all[j]
            loss_tot[...] = tot

        @pl.when(s < last)
        def _():
            pltpu.make_async_copy(loss_tot, loss_tot, ltot_rsem).wait()

        @pl.when(s > 0)
        def _():
            pltpu.make_async_remote_copy(
                src_ref=loss_tot, dst_ref=loss_tot, send_sem=loss_ssem.at[1], recv_sem=ltot_rsem,
                device_id={"pp": s - 1, "tp": t}, device_id_type=pl.DeviceIdType.MESH).start()

    def bwd_a(layer, m):
        lp = 2 + layer
        rows = rows_of(m)
        if layer == 1:
            wait_slices(dh_buf, 1, 3, m, True)
        else:
            @pl.when(s < away)
            def _():
                wait_slices(dh_buf, 0, 2, m, False)

            @pl.when(s >= away)
            def _():
                wait_slices(dh_buf, 0, 2, m, True)
        for c in range(hidden // hc):
            cols = slice(c * hc, (c + 1) * hc)
            acc = dot_t(dh_buf[layer, 0, rows, :], w2[layer, 0, cols, :])
            for j in range(1, n_tp):
                acc = acc + dot_t(dh_buf[layer, j, rows, :], w2[layer, j, cols, :])
            u = u_buf[layer, rows, cols].astype(F32)
            g_buf[layer, rows, cols] = (gelu_grad(u) * acc).astype(BF16)

        def send():
            partials(lp, m, dh_buf, layer, lambda j: dot_t(
                g_buf[layer, rows, :], w1[layer, pl.ds(pl.multiple_of(j * ds, ds), ds), :]))

        if layer == 1:
            send()
        else:
            pl.when(s > 0)(send)
        copy_out_slices(dh_buf, dh_out, layer, m, out_sem.at[2 + layer])
        pltpu.make_async_copy(g_buf.at[layer, rows], g_out.at[layer, rows], out_sem.at[6 + layer]).start()
        if layer == 1:
            pl.when(m == n_mb - 1)(pass_loss)

    def bwd_b(layer, m):
        lp = 2 + layer
        rows = rows_of(m)
        h = reduce_own(lp, m)
        hs_send[lp, rows, :] = h
        if layer == 1:
            for d in far_first:
                send_slice(lp, dh_buf, 0, 2, s, d, m)
            dh_buf[0, t, rows, :] = h
        else:
            for d in far_first + (0,):
                send_slice(lp, dh_buf, 1, 3, s - 1, d, m)

    def bwd_b_guest(layer, m):
        lp = 2 + layer
        rows = rows_of(m)
        guest_send[lp, rows, :] = reduce_guest(lp, m)
        if layer == 1:
            send_guest(lp, dh_buf, 0, 2, last, m)
        else:
            send_guest(lp, dh_buf, 1, 3, last - 1, m)

    f_start = 4 * s
    b_start = 2 * n_layer + shift + 4 * (last - s)

    def tick(k, carry):
        @pl.when(k == 1)
        def _():
            for c in loads[1]:
                c.wait()

        bias = 8 * n_pp + 2 * n_layer + shift + 4 + spacing
        bias = spacing * (-(-bias // spacing))
        turn = {}
        for name, start in (("f", f_start), ("b", b_start)):
            q = k - start + bias
            turn[name] = (lax.div(q, spacing) - bias // spacing, lax.rem(q, spacing) if spacing > 1 else None)

        def at(name, offset, fn, layer, extra=None):
            m, phase = turn[name]
            m = m - offset // spacing
            ok = (m >= 0) & (m < n_mb)
            if phase is not None:
                ok = ok & (phase == offset % spacing)
            if extra is not None:
                ok = ok & extra
            pl.when(ok)(lambda: fn(layer, m))

        here, host, far = s < away, s == host_stage, 4 * (last - host_stage)
        at("b", 3, bwd_b, 0, here & (s > 0))
        at("b", 3 - far, bwd_b_guest, 0, host)
        at("b", 2, bwd_a, 0)
        at("b", 1, bwd_b, 1, here)
        at("b", 1 - far, bwd_b_guest, 1, host)
        at("b", 0, bwd_a, 1)
        at("f", 3, fwd_b, 1, here)
        at("f", 3 + far, fwd_b_guest, 1, host)
        at("f", 2, fwd_a, 1)
        at("f", 1, fwd_b, 0, here)
        at("f", 1 + far, fwd_b_guest, 0, host)
        at("f", 0, fwd_a, 0)
        return carry

    n_ticks = 4 * n_layer + shift + spacing * (n_mb - 1)
    lax.fori_loop(0, n_ticks, tick, 0)

    for layer in range(2):
        for i in range(4):
            pltpu.make_async_copy(z_buf.at[layer], z_out.at[layer], out_sem.at[2 * i + layer]).wait()

    def wait_three(sem):
        pltpu.make_async_copy(rs_send.at[0], rs_send.at[0], sem).wait()

    def wait_four(sem):
        pltpu.make_async_copy(a_buf.at[0], a_buf.at[0], sem).wait()

    for lp in (0, 1, 3):
        wait_three(rs_ssem.at[lp])

    @pl.when(s < away)
    def _():
        wait_three(ag_ssem.at[0])
        wait_three(ag_ssem.at[3])
        wait_four(ag_ssem.at[1])

    @pl.when((s < away) & (s > 0))
    def _():
        wait_four(ag_ssem.at[2])

    @pl.when(s >= away)
    def _():
        for lp in range(4):
            pltpu.make_async_copy(own_send.at[lp], own_send.at[lp], own_ssem.at[lp]).wait()

    @pl.when(s == host_stage)
    def _():
        for lp in range(4):
            wait_four(guest_ssem.at[lp])

    @pl.when(s == host_stage)
    def _():
        pltpu.make_async_copy(loss_all, loss_all, loss_ssem.at[0]).wait()

    @pl.when(s > 0)
    def _():
        wait_three(rs_ssem.at[2])
        pltpu.make_async_copy(loss_tot, loss_tot, loss_ssem.at[1]).wait()

    loss_out[...] = loss_tot[...]


def dot_tokens(a, b):
    return lax.dot_general(a, b, (((0,), (0,)), ((), ())), preferred_element_type=F32)


def grad_kernel(inv_count, a_ref, g_ref, z_ref, dh_ref, loss_ref, first_ref, second_ref, total_ref):
    @pl.when((pl.program_id(0) == 0) & (pl.program_id(1) == 0))
    def _():
        total_ref[0, 0] = jnp.sum(loss_ref[...]) * inv_count

    first_ref[0] = dot_tokens(a_ref[0], g_ref[0])
    second_ref[0] = dot_tokens(z_ref[0], dh_ref[0])


def weight_grads(a, g, z, dh, loss, inv_count):
    n_layer, n_tok, d_model = a.shape
    hidden = g.shape[2]
    steps = d_model // GRAD_TILE
    rows2 = hidden // steps
    return pl.pallas_call(
        functools.partial(grad_kernel, inv_count),
        grid=(n_layer, steps),
        in_specs=[
            pl.BlockSpec((1, n_tok, GRAD_TILE), lambda l, j: (l, 0, j)),
            pl.BlockSpec((1, n_tok, hidden), lambda l, j: (l, 0, 0)),
            pl.BlockSpec((1, n_tok, rows2), lambda l, j: (l, 0, j)),
            pl.BlockSpec((1, n_tok, d_model), lambda l, j: (l, 0, 0)),
            pl.BlockSpec((8, 128), lambda l, j: (0, 0)),
        ],
        out_specs=[
            pl.BlockSpec((1, GRAD_TILE, hidden), lambda l, j: (l, j, 0)),
            pl.BlockSpec((1, rows2, d_model), lambda l, j: (l, j, 0)),
            pl.BlockSpec(memory_space=pltpu.SMEM),
        ],
        out_shape=[
            jax.ShapeDtypeStruct((n_layer, d_model, hidden), F32),
            jax.ShapeDtypeStruct((n_layer, hidden, d_model), F32),
            jax.ShapeDtypeStruct((1, 1), F32),
        ],
        compiler_params=pltpu.CompilerParams(vmem_limit_bytes=63 * 1024 * 1024),
        cost_estimate=pl.CostEstimate(
            flops=8 * n_tok * d_model * hidden, bytes_accessed=4 * n_layer * 2 * n_tok * d_model * 2, transcendentals=0),
        name="weight_grads",
    )(a, g, z, dh, loss)


def solution(mesh):
    n_pp = mesh.shape["pp"]
    n_tp = mesh.shape["tp"]

    def device_program(x_loc, y_loc, w_in, w_out):
        n_tok = x_loc.shape[0] * x_loc.shape[1]
        d_model = x_loc.shape[2]
        hidden = w_in.shape[3]
        ds = d_model // n_tp
        rows_mb = CHUNK
        n_mb = n_tok // rows_mb
        inv_count = 1.0 / (n_tok * d_model)
        kernel = functools.partial(stack_kernel, n_pp, n_tp, rows_mb, SPACING, SHIFT, inv_count)
        any_spec = pl.BlockSpec(memory_space=pl.ANY)
        dma = pltpu.SemaphoreType.DMA
        a, dh, z, g, loss = pl.pallas_call(
            kernel,
            out_shape=[
                jax.ShapeDtypeStruct((2, n_tok, d_model), BF16),
                jax.ShapeDtypeStruct((2, n_tok, d_model), BF16),
                jax.ShapeDtypeStruct((2, n_tok, hidden), BF16),
                jax.ShapeDtypeStruct((2, n_tok, hidden), BF16),
                jax.ShapeDtypeStruct((8, 128), F32),
            ],
            in_specs=[any_spec] * 4,
            out_specs=[any_spec] * 4 + [pl.BlockSpec(memory_space=pltpu.VMEM)],
            scratch_shapes=[
                pltpu.VMEM((2, d_model, hidden), BF16),
                pltpu.VMEM((2, n_tp, hidden, ds), BF16),
                pltpu.VMEM((2, n_tp, n_tok, ds), BF16),
                pltpu.VMEM((2, n_tp, n_tok, ds), BF16),
                pltpu.VMEM((2, n_tok, hidden), BF16),
                pltpu.VMEM((2, n_tok, hidden), BF16),
                pltpu.VMEM((2, n_tok, hidden), BF16),
                pltpu.VMEM((4, 3, n_tok, ds), BF16),
                pltpu.VMEM((4, 3, n_tok, ds), BF16),
                pltpu.VMEM((4, n_tok, ds), BF16),
                pltpu.VMEM((4, rows_mb, ds), F32),
                pltpu.VMEM((n_tok, ds), BF16),
                pltpu.VMEM((8, 128), F32),
                pltpu.VMEM((n_tp, 8, 128), F32),
                pltpu.VMEM((8, 128), F32),
                pltpu.VMEM((4, 3, n_tok, ds), BF16),
                pltpu.VMEM((4, n_tok, ds), F32),
                pltpu.VMEM((4, n_tok, ds), F32),
                pltpu.VMEM((4, n_tok, ds), BF16),
                dma((3 + 3 * n_tp,)),
                dma((4, 3, n_mb)),
                dma((4, n_tp, n_mb)),
                dma((4,)),
                dma((4,)),
                dma((8,)),
                dma((4, 4, n_mb)),
                dma((4,)),
                dma((4,)),
                dma((n_tp,)),
                dma,
                dma((2,)),
            ],
            compiler_params=pltpu.CompilerParams(has_side_effects=True, vmem_limit_bytes=63 * 1024 * 1024),
            cost_estimate=pl.CostEstimate(flops=10**11, bytes_accessed=10**8, transcendentals=0),
            name="mlp_stack",
        )(x_loc.reshape(n_tok, d_model), y_loc.reshape(n_tok, d_model), w_in[0], w_out[0])
        grad_first, grad_second, loss_val = weight_grads(a, g, z, dh, loss, inv_count)
        grad_first, grad_second = grad_first[None], grad_second[None]
        return grad_first, grad_second, loss_val.reshape(1)

    return jax.shard_map(
        device_program,
        mesh=mesh,
        in_specs=(P("dp", None, None), P("dp", None, None), P("pp", None, None, "tp"), P("pp", None, "tp", None)),
        out_specs=(P(("dp", "pp"), None, None, "tp"), P(("dp", "pp"), None, "tp", None), P("dp")),
        check_vma=False,
    )
```

```python
import functools
import math

import jax
import jax.numpy as jnp
from jax import lax
from jax.experimental import pallas as pl
from jax.experimental.pallas import tpu as pltpu
from jax.sharding import PartitionSpec as P

F32 = jnp.float32
BF16 = jnp.bfloat16
CHUNK = 64
SPACING = 1
HOST = 1
GRAD_TILE = 512
SHIFT = 0
GELU_C = math.sqrt(2.0 / math.pi)
GELU_K = 0.044715


def gelu_fwd(u):
    return 0.5 * u * (1.0 + jnp.tanh(GELU_C * (u + GELU_K * (u * u * u))))


def gelu_grad(u):
    sq = u * u
    th = jnp.tanh(GELU_C * (u + GELU_K * (sq * u)))
    return 0.5 * (1.0 + th) + (0.5 * GELU_C) * u * (1.0 - th * th) * (1.0 + (3.0 * GELU_K) * sq)


def dot(a, b):
    return jnp.dot(a, b, preferred_element_type=F32)


def dot_t(a, b):
    return lax.dot_general(a, b, (((1,), (1,)), ((), ())), preferred_element_type=F32)


def stack_kernel(n_pp, n_tp, rows_mb, spacing, shift, inv_count,
                 x_hbm, y_hbm, w1_hbm, w2_hbm,
                 a_out, dh_out, z_out, g_out, loss_out,
                 w1, w2, a_buf, dh_buf, u_buf, z_buf, g_buf, rs_recv, rs_send, hs_send,
                 own_part, t_buf, loss_acc, loss_all, loss_tot,
                 guest_own, own_send, guest_send,
                 load_sem, rs_rsem, ag_rsem, rs_ssem, ag_ssem, out_sem,
                 guest_rsem, guest_ssem, own_ssem,
                 lall_rsem, ltot_rsem, loss_ssem):
    t = lax.axis_index("tp")
    s = lax.axis_index("pp")
    last = n_pp - 1
    away = last
    host_stage = HOST
    n_tok = a_buf.shape[2]
    ds = a_buf.shape[3]
    hidden = w1.shape[2]
    n_mb = n_tok // rows_mb
    n_layer = 2 * n_pp
    hc = 512

    def peer(d):
        return lax.rem(t + d, n_tp)

    far_first = (2, 1, 3)

    loads = [[], []]
    for layer in range(2):
        loads[layer].append(pltpu.make_async_copy(w1_hbm.at[layer], w1.at[layer], load_sem.at[layer]))
        for j in range(n_tp):
            loads[layer].append(pltpu.make_async_copy(
                w2_hbm.at[layer, :, pl.ds(j * ds, ds)], w2.at[layer, j], load_sem.at[2 + layer * n_tp + j]))
    def x_load(j, first, rows, sem):
        return pltpu.make_async_copy(
            x_hbm.at[pl.ds(first, rows), pl.ds(j * ds, ds)], a_buf.at[0, j, pl.ds(first, rows)], load_sem.at[sem + j])

    x_head = [x_load(j, 0, rows_mb, 2 + 2 * n_tp) for j in range(n_tp)]
    x_tail = [x_load(j, rows_mb, n_tok - rows_mb, 2 + 3 * n_tp) for j in range(n_tp)]
    y_load = pltpu.make_async_copy(
        y_hbm.at[:, pl.ds(pl.multiple_of(t * ds, ds), ds)], t_buf, load_sem.at[2 + 4 * n_tp])

    @pl.when(s == 0)
    def _():
        for c in x_head:
            c.start()

    for c in loads[0]:
        c.start()

    @pl.when(s == host_stage)
    def _():
        loss_acc[...] = jnp.zeros_like(loss_acc)

    @pl.when(s == 0)
    def _():
        for c in x_head:
            c.wait()

    for c in loads[0]:
        c.wait()
    for c in loads[1]:
        c.start()
    pl.when(s == 0)(lambda: [c.start() for c in x_tail] and None)
    pl.when(s == host_stage)(y_load.start)

    def rows_of(m):
        return pl.ds(pl.multiple_of(m * rows_mb, rows_mb), rows_mb)

    def wait_slices(buf, layer, lp, m, with_own):
        rows = rows_of(m)
        for d in ((0,) if with_own else ()) + (1, 3, 2):
            j = peer(d)
            ref = buf.at[layer, j, rows]
            pltpu.make_async_copy(ref, ref, ag_rsem.at[lp, j, m]).wait()

    def copy_out_slices(buf, out, layer, m, sem):
        rows = rows_of(m)
        for j in range(n_tp):
            pltpu.make_async_copy(buf.at[layer, j, rows], out.at[layer, rows, pl.ds(j * ds, ds)], sem).start()

    moved = lax.div(s, last)
    reducer = s + moved * (host_stage - last)

    def send_part(lp, d, m):
        rows = rows_of(m)
        pltpu.make_async_remote_copy(
            src_ref=rs_send.at[lp, d - 1, rows], dst_ref=rs_recv.at[moved, lp, d - 1, rows],
            send_sem=rs_ssem.at[lp], recv_sem=rs_rsem.at[moved, lp, d - 1, m],
            device_id={"pp": reducer, "tp": peer(d)}, device_id_type=pl.DeviceIdType.MESH).start()

    def send_slice(lp, buf, layer, lp_dst, stage, d, m):
        rows = rows_of(m)
        pltpu.make_async_remote_copy(
            src_ref=hs_send.at[lp, rows], dst_ref=buf.at[layer, t, rows],
            send_sem=ag_ssem.at[lp], recv_sem=ag_rsem.at[lp_dst, t, m],
            device_id={"pp": stage, "tp": peer(d)}, device_id_type=pl.DeviceIdType.MESH).start()

    def send_guest(lp, buf, layer, lp_dst, stage, m):
        rows = rows_of(m)
        for d in far_first + (0,):
            pltpu.make_async_remote_copy(
                src_ref=guest_send.at[lp, rows], dst_ref=buf.at[layer, t, rows],
                send_sem=guest_ssem.at[lp], recv_sem=ag_rsem.at[lp_dst, t, m],
                device_id={"pp": stage, "tp": peer(d)}, device_id_type=pl.DeviceIdType.MESH).start()

    def partials(lp, m, buf, layer, farthest, fn):
        rows = rows_of(m)
        for d in far_first:
            part = farthest if d == far_first[0] else fn(peer(d))
            rs_send[lp, d - 1, rows, :] = part.astype(BF16)
            send_part(lp, d, m)
        own = buf[layer, t, rows, :].astype(F32) + fn(t)

        @pl.when(s < away)
        def _():
            own_part[lp] = own

        @pl.when(s >= away)
        def _():
            own_send[lp, rows, :] = own
            pltpu.make_async_remote_copy(
                src_ref=own_send.at[lp, rows], dst_ref=guest_own.at[lp, rows],
                send_sem=own_ssem.at[lp], recv_sem=guest_rsem.at[lp, m],
                device_id={"pp": host_stage, "tp": t}, device_id_type=pl.DeviceIdType.MESH).start()

    def reduce_own(lp, m):
        rows = rows_of(m)
        for d in (1, 3, 2):
            ref = rs_recv.at[0, lp, d - 1, rows]
            pltpu.make_async_copy(ref, ref, rs_rsem.at[0, lp, d - 1, m]).wait()
        acc = own_part[lp]
        for d in (1, 3, 2):
            acc = acc + rs_recv[0, lp, d - 1, rows, :].astype(F32)
        return acc.astype(BF16)

    def reduce_guest(lp, m):
        rows = rows_of(m)
        for d in (1, 3, 2):
            ref = rs_recv.at[1, lp, d - 1, rows]
            pltpu.make_async_copy(ref, ref, rs_rsem.at[1, lp, d - 1, m]).wait()
        ref = guest_own.at[lp, rows]
        pltpu.make_async_copy(ref, ref, guest_rsem.at[lp, m]).wait()
        acc = guest_own[lp, rows, :]
        for d in (1, 3, 2):
            acc = acc + rs_recv[1, lp, d - 1, rows, :].astype(F32)
        return acc.astype(BF16)

    def fwd_a(layer, m):
        rows = rows_of(m)
        if layer == 0:
            @pl.when(s > 0)
            def _():
                wait_slices(a_buf, 0, 0, m, True)
        else:
            @pl.when(s < away)
            def _():
                wait_slices(a_buf, 1, 1, m, False)

            @pl.when(s >= away)
            def _():
                wait_slices(a_buf, 1, 1, m, True)
        for c in range(hidden // hc):
            cols = slice(c * hc, (c + 1) * hc)
            acc = dot(a_buf[layer, 0, rows, :], w1[layer, 0:ds, cols])
            for j in range(1, n_tp):
                acc = acc + dot(a_buf[layer, j, rows, :], w1[layer, j * ds:(j + 1) * ds, cols])
            u = acc.astype(BF16)
            u_buf[layer, rows, cols] = u
            z = gelu_fwd(u.astype(F32)).astype(BF16)
            z_buf[layer, rows, cols] = z
            part = dot(z, w2[layer, peer(far_first[0]), cols, :])
            farthest = part if c == 0 else farthest + part
        partials(layer, m, a_buf, layer, farthest, lambda j: dot(z_buf[layer, rows, :], w2[layer, j]))
        copy_out_slices(a_buf, a_out, layer, m, out_sem.at[layer])
        pltpu.make_async_copy(z_buf.at[layer, rows], z_out.at[layer, rows], out_sem.at[4 + layer]).start()

    def fwd_b(layer, m):
        rows = rows_of(m)
        h = reduce_own(layer, m)
        hs_send[layer, rows, :] = h
        if layer == 0:
            for d in far_first:
                send_slice(0, a_buf, 1, 1, s, d, m)
            a_buf[1, t, rows, :] = h
        else:
            for d in far_first + (0,):
                send_slice(1, a_buf, 0, 0, s + 1, d, m)

    def fwd_b_guest(layer, m):
        rows = rows_of(m)
        h = reduce_guest(layer, m)
        if layer == 0:
            guest_send[0, rows, :] = h
            send_guest(0, a_buf, 1, 1, last, m)
            return
        err = h.astype(F32) - t_buf[rows, :].astype(F32)
        guest_send[1, rows, :] = (err * inv_count).astype(BF16)
        send_guest(1, dh_buf, 1, 3, last, m)
        half = 0.5 * err * err
        half = jnp.sum(half.reshape(rows_mb // 8, 8, ds), axis=0)
        part = half[:, :128]
        for q in range(1, ds // 128):
            part = part + half[:, q * 128:(q + 1) * 128]
        loss_acc[...] = loss_acc[...] + part

        @pl.when(m == n_mb - 1)
        def _():
            for d in far_first + (0,):
                pltpu.make_async_remote_copy(
                    src_ref=loss_acc, dst_ref=loss_all.at[t],
                    send_sem=loss_ssem.at[0], recv_sem=lall_rsem.at[t],
                    device_id={"pp": last, "tp": peer(d)}, device_id_type=pl.DeviceIdType.MESH).start()

    def pass_loss():
        @pl.when(s == last)
        def _():
            for j in range(n_tp):
                pltpu.make_async_copy(loss_all.at[j], loss_all.at[j], lall_rsem.at[j]).wait()
            tot = loss_all[0]
            for j in range(1, n_tp):
                tot = tot + loss_all[j]
            loss_tot[...] = tot

        @pl.when(s < last)
        def _():
            pltpu.make_async_copy(loss_tot, loss_tot, ltot_rsem).wait()

        @pl.when(s > 0)
        def _():
            pltpu.make_async_remote_copy(
                src_ref=loss_tot, dst_ref=loss_tot, send_sem=loss_ssem.at[1], recv_sem=ltot_rsem,
                device_id={"pp": s - 1, "tp": t}, device_id_type=pl.DeviceIdType.MESH).start()

    def bwd_a(layer, m):
        lp = 2 + layer
        rows = rows_of(m)
        if layer == 1:
            wait_slices(dh_buf, 1, 3, m, True)
        else:
            @pl.when(s < away)
            def _():
                wait_slices(dh_buf, 0, 2, m, False)

            @pl.when(s >= away)
            def _():
                wait_slices(dh_buf, 0, 2, m, True)
        far_rows = pl.ds(pl.multiple_of(peer(far_first[0]) * ds, ds), ds)
        for c in range(hidden // hc):
            cols = slice(c * hc, (c + 1) * hc)
            acc = dot_t(dh_buf[layer, 0, rows, :], w2[layer, 0, cols, :])
            for j in range(1, n_tp):
                acc = acc + dot_t(dh_buf[layer, j, rows, :], w2[layer, j, cols, :])
            u = u_buf[layer, rows, cols].astype(F32)
            g = (gelu_grad(u) * acc).astype(BF16)
            g_buf[layer, rows, cols] = g
            part = dot_t(g, w1[layer, far_rows, cols])
            farthest = part if c == 0 else farthest + part

        def send():
            partials(lp, m, dh_buf, layer, farthest, lambda j: dot_t(
                g_buf[layer, rows, :], w1[layer, pl.ds(pl.multiple_of(j * ds, ds), ds), :]))

        if layer == 1:
            send()
        else:
            pl.when(s > 0)(send)
        copy_out_slices(dh_buf, dh_out, layer, m, out_sem.at[2 + layer])
        pltpu.make_async_copy(g_buf.at[layer, rows], g_out.at[layer, rows], out_sem.at[6 + layer]).start()
        if layer == 1:
            pl.when(m == n_mb - 1)(pass_loss)

    def bwd_b(layer, m):
        lp = 2 + layer
        rows = rows_of(m)
        h = reduce_own(lp, m)
        hs_send[lp, rows, :] = h
        if layer == 1:
            for d in far_first:
                send_slice(lp, dh_buf, 0, 2, s, d, m)
            dh_buf[0, t, rows, :] = h
        else:
            for d in far_first + (0,):
                send_slice(lp, dh_buf, 1, 3, s - 1, d, m)

    def bwd_b_guest(layer, m):
        lp = 2 + layer
        rows = rows_of(m)
        guest_send[lp, rows, :] = reduce_guest(lp, m)
        if layer == 1:
            send_guest(lp, dh_buf, 0, 2, last, m)
        else:
            send_guest(lp, dh_buf, 1, 3, last - 1, m)

    f_start = 4 * s
    b_start = 2 * n_layer + shift + 4 * (last - s)

    def tick(k, carry):
        @pl.when(k == 1)
        def _():
            for c in loads[1]:
                c.wait()

        @pl.when((k == 1) & (s == 0))
        def _():
            for c in x_tail:
                c.wait()

        @pl.when((k == 1) & (s == host_stage))
        def _():
            y_load.wait()

        bias = 8 * n_pp + 2 * n_layer + shift + 4 + spacing
        bias = spacing * (-(-bias // spacing))
        turn = {}
        for name, start in (("f", f_start), ("b", b_start)):
            q = k - start + bias
            turn[name] = (lax.div(q, spacing) - bias // spacing, lax.rem(q, spacing) if spacing > 1 else None)

        def at(name, offset, fn, layer, extra=None):
            m, phase = turn[name]
            m = m - offset // spacing
            ok = (m >= 0) & (m < n_mb)
            if phase is not None:
                ok = ok & (phase == offset % spacing)
            if extra is not None:
                ok = ok & extra
            pl.when(ok)(lambda: fn(layer, m))

        here, host, far = s < away, s == host_stage, 4 * (last - host_stage)
        at("b", 3, bwd_b, 0, here & (s > 0))
        at("b", 3 - far, bwd_b_guest, 0, host)
        at("b", 2, bwd_a, 0)
        at("b", 1, bwd_b, 1, here)
        at("b", 1 - far, bwd_b_guest, 1, host)
        at("b", 0, bwd_a, 1)
        at("f", 3, fwd_b, 1, here)
        at("f", 3 + far, fwd_b_guest, 1, host)
        at("f", 2, fwd_a, 1)
        at("f", 1, fwd_b, 0, here)
        at("f", 1 + far, fwd_b_guest, 0, host)
        at("f", 0, fwd_a, 0)
        return carry

    n_ticks = 4 * n_layer + shift + spacing * (n_mb - 1)
    lax.fori_loop(0, n_ticks, tick, 0)

    for layer in range(2):
        for i in range(4):
            pltpu.make_async_copy(z_buf.at[layer], z_out.at[layer], out_sem.at[2 * i + layer]).wait()

    def wait_three(sem):
        pltpu.make_async_copy(rs_send.at[0], rs_send.at[0], sem).wait()

    def wait_four(sem):
        pltpu.make_async_copy(a_buf.at[0], a_buf.at[0], sem).wait()

    for lp in (0, 1, 3):
        wait_three(rs_ssem.at[lp])

    @pl.when(s < away)
    def _():
        wait_three(ag_ssem.at[0])
        wait_three(ag_ssem.at[3])
        wait_four(ag_ssem.at[1])

    @pl.when((s < away) & (s > 0))
    def _():
        wait_four(ag_ssem.at[2])

    @pl.when(s >= away)
    def _():
        for lp in range(4):
            pltpu.make_async_copy(own_send.at[lp], own_send.at[lp], own_ssem.at[lp]).wait()

    @pl.when(s == host_stage)
    def _():
        for lp in range(4):
            wait_four(guest_ssem.at[lp])

    @pl.when(s == host_stage)
    def _():
        pltpu.make_async_copy(loss_all, loss_all, loss_ssem.at[0]).wait()

    @pl.when(s > 0)
    def _():
        wait_three(rs_ssem.at[2])
        pltpu.make_async_copy(loss_tot, loss_tot, loss_ssem.at[1]).wait()

    loss_out[...] = loss_tot[...]


def dot_tokens(a, b):
    return lax.dot_general(a, b, (((0,), (0,)), ((), ())), preferred_element_type=F32)


def grad_kernel(inv_count, a_ref, g_ref, z_ref, dh_ref, loss_ref, first_ref, second_ref, total_ref):
    @pl.when((pl.program_id(0) == 0) & (pl.program_id(1) == 0))
    def _():
        total_ref[0, 0] = jnp.sum(loss_ref[...]) * inv_count

    first_ref[0] = dot_tokens(a_ref[0], g_ref[0])
    second_ref[0] = dot_tokens(z_ref[0], dh_ref[0])


def weight_grads(a, g, z, dh, loss, inv_count):
    n_layer, n_tok, d_model = a.shape
    hidden = g.shape[2]
    steps = d_model // GRAD_TILE
    rows2 = hidden // steps
    return pl.pallas_call(
        functools.partial(grad_kernel, inv_count),
        grid=(n_layer, steps),
        in_specs=[
            pl.BlockSpec((1, n_tok, GRAD_TILE), lambda l, j: (l, 0, j)),
            pl.BlockSpec((1, n_tok, hidden), lambda l, j: (l, 0, 0)),
            pl.BlockSpec((1, n_tok, rows2), lambda l, j: (l, 0, j)),
            pl.BlockSpec((1, n_tok, d_model), lambda l, j: (l, 0, 0)),
            pl.BlockSpec((8, 128), lambda l, j: (0, 0)),
        ],
        out_specs=[
            pl.BlockSpec((1, GRAD_TILE, hidden), lambda l, j: (l, j, 0)),
            pl.BlockSpec((1, rows2, d_model), lambda l, j: (l, j, 0)),
            pl.BlockSpec(memory_space=pltpu.SMEM),
        ],
        out_shape=[
            jax.ShapeDtypeStruct((n_layer, d_model, hidden), F32),
            jax.ShapeDtypeStruct((n_layer, hidden, d_model), F32),
            jax.ShapeDtypeStruct((1, 1), F32),
        ],
        compiler_params=pltpu.CompilerParams(vmem_limit_bytes=63 * 1024 * 1024),
        cost_estimate=pl.CostEstimate(
            flops=8 * n_tok * d_model * hidden, bytes_accessed=4 * n_layer * 2 * n_tok * d_model * 2, transcendentals=0),
        name="weight_grads",
    )(a, g, z, dh, loss)


def solution(mesh):
    n_pp = mesh.shape["pp"]
    n_tp = mesh.shape["tp"]

    def device_program(x_loc, y_loc, w_in, w_out):
        n_tok = x_loc.shape[0] * x_loc.shape[1]
        d_model = x_loc.shape[2]
        hidden = w_in.shape[3]
        ds = d_model // n_tp
        rows_mb = CHUNK
        n_mb = n_tok // rows_mb
        inv_count = 1.0 / (n_tok * d_model)
        kernel = functools.partial(stack_kernel, n_pp, n_tp, rows_mb, SPACING, SHIFT, inv_count)
        any_spec = pl.BlockSpec(memory_space=pl.ANY)
        dma = pltpu.SemaphoreType.DMA
        a, dh, z, g, loss = pl.pallas_call(
            kernel,
            out_shape=[
                jax.ShapeDtypeStruct((2, n_tok, d_model), BF16),
                jax.ShapeDtypeStruct((2, n_tok, d_model), BF16),
                jax.ShapeDtypeStruct((2, n_tok, hidden), BF16),
                jax.ShapeDtypeStruct((2, n_tok, hidden), BF16),
                jax.ShapeDtypeStruct((8, 128), F32),
            ],
            in_specs=[any_spec] * 4,
            out_specs=[any_spec] * 4 + [pl.BlockSpec(memory_space=pltpu.VMEM)],
            scratch_shapes=[
                pltpu.VMEM((2, d_model, hidden), BF16),
                pltpu.VMEM((2, n_tp, hidden, ds), BF16),
                pltpu.VMEM((2, n_tp, n_tok, ds), BF16),
                pltpu.VMEM((2, n_tp, n_tok, ds), BF16),
                pltpu.VMEM((2, n_tok, hidden), BF16),
                pltpu.VMEM((2, n_tok, hidden), BF16),
                pltpu.VMEM((2, n_tok, hidden), BF16),
                pltpu.VMEM((2, 4, 3, n_tok, ds), BF16),
                pltpu.VMEM((4, 3, n_tok, ds), BF16),
                pltpu.VMEM((4, n_tok, ds), BF16),
                pltpu.VMEM((4, rows_mb, ds), F32),
                pltpu.VMEM((n_tok, ds), BF16),
                pltpu.VMEM((8, 128), F32),
                pltpu.VMEM((n_tp, 8, 128), F32),
                pltpu.VMEM((8, 128), F32),
                pltpu.VMEM((4, n_tok, ds), F32),
                pltpu.VMEM((4, n_tok, ds), F32),
                pltpu.VMEM((4, n_tok, ds), BF16),
                dma((3 + 4 * n_tp,)),
                dma((2, 4, 3, n_mb)),
                dma((4, n_tp, n_mb)),
                dma((4,)),
                dma((4,)),
                dma((8,)),
                dma((4, n_mb)),
                dma((4,)),
                dma((4,)),
                dma((n_tp,)),
                dma,
                dma((2,)),
            ],
            compiler_params=pltpu.CompilerParams(has_side_effects=True, vmem_limit_bytes=63 * 1024 * 1024),
            cost_estimate=pl.CostEstimate(flops=10**11, bytes_accessed=10**8, transcendentals=0),
            name="mlp_stack",
        )(x_loc.reshape(n_tok, d_model), y_loc.reshape(n_tok, d_model), w_in[0], w_out[0])
        grad_first, grad_second, loss_val = weight_grads(a, g, z, dh, loss, inv_count)
        grad_first, grad_second = grad_first[None], grad_second[None]
        return grad_first, grad_second, loss_val.reshape(1)

    return jax.shard_map(
        device_program,
        mesh=mesh,
        in_specs=(P("dp", None, None), P("dp", None, None), P("pp", None, None, "tp"), P("pp", None, "tp", None)),
        out_specs=(P(("dp", "pp"), None, None, "tp"), P(("dp", "pp"), None, "tp", None), P("dp")),
        check_vma=False,
    )
```

```python
import functools
import math

import jax
import jax.numpy as jnp
from jax import lax
from jax.experimental import pallas as pl
from jax.experimental.pallas import tpu as pltpu
from jax.sharding import PartitionSpec as P

F32 = jnp.float32
BF16 = jnp.bfloat16
CHUNK = 64
SPACING = 1
HOST = 1
GRAD_TILE = 512
SHIFT = 0
GELU_C = math.sqrt(2.0 / math.pi)
GELU_K = 0.044715


def gelu_fwd(u):
    return 0.5 * u * (1.0 + jnp.tanh(GELU_C * (u + GELU_K * (u * u * u))))


def gelu_grad(u):
    sq = u * u
    th = jnp.tanh(GELU_C * (u + GELU_K * (sq * u)))
    return 0.5 * (1.0 + th) + (0.5 * GELU_C) * u * (1.0 - th * th) * (1.0 + (3.0 * GELU_K) * sq)


def dot(a, b):
    return jnp.dot(a, b, preferred_element_type=F32)


def dot_t(a, b):
    return lax.dot_general(a, b, (((1,), (1,)), ((), ())), preferred_element_type=F32)


def stack_kernel(n_pp, n_tp, rows_mb, spacing, shift, inv_count,
                 x_hbm, y_hbm, w1_hbm, w2_hbm,
                 a_out, dh_out, z_out, g_out, loss_out,
                 w1, w2, a_buf, dh_buf, slope_buf, z_buf, g_buf, rs_recv, rs_send, hs_send,
                 own_part, t_buf, loss_acc, loss_all, loss_tot,
                 guest_own, own_send, guest_send,
                 load_sem, rs_rsem, ag_rsem, rs_ssem, ag_ssem, out_sem,
                 guest_rsem, guest_ssem, own_ssem,
                 lall_rsem, ltot_rsem, loss_ssem):
    t = lax.axis_index("tp")
    s = lax.axis_index("pp")
    last = n_pp - 1
    away = last
    host_stage = HOST
    n_tok = a_buf.shape[2]
    ds = a_buf.shape[3]
    hidden = w1.shape[2]
    n_mb = n_tok // rows_mb
    n_layer = 2 * n_pp
    hc = 512

    def peer(d):
        return lax.rem(t + d, n_tp)

    far_first = (2, 1, 3)

    loads = [[], []]
    for layer in range(2):
        loads[layer].append(pltpu.make_async_copy(w1_hbm.at[layer], w1.at[layer], load_sem.at[layer]))
        for j in range(n_tp):
            loads[layer].append(pltpu.make_async_copy(
                w2_hbm.at[layer, :, pl.ds(j * ds, ds)], w2.at[layer, j], load_sem.at[2 + layer * n_tp + j]))
    def x_load(j, first, rows, sem):
        return pltpu.make_async_copy(
            x_hbm.at[pl.ds(first, rows), pl.ds(j * ds, ds)], a_buf.at[0, j, pl.ds(first, rows)], load_sem.at[sem + j])

    x_head = [x_load(j, 0, rows_mb, 2 + 2 * n_tp) for j in range(n_tp)]
    x_tail = [x_load(j, rows_mb, n_tok - rows_mb, 2 + 3 * n_tp) for j in range(n_tp)]
    y_load = pltpu.make_async_copy(
        y_hbm.at[:, pl.ds(pl.multiple_of(t * ds, ds), ds)], t_buf, load_sem.at[2 + 4 * n_tp])

    @pl.when(s == 0)
    def _():
        for c in x_head:
            c.start()

    for c in loads[0]:
        c.start()

    @pl.when(s == host_stage)
    def _():
        loss_acc[...] = jnp.zeros_like(loss_acc)

    @pl.when(s == 0)
    def _():
        for c in x_head:
            c.wait()

    for c in loads[0]:
        c.wait()
    for c in loads[1]:
        c.start()
    pl.when(s == 0)(lambda: [c.start() for c in x_tail] and None)
    pl.when(s == host_stage)(y_load.start)

    def rows_of(m):
        return pl.ds(pl.multiple_of(m * rows_mb, rows_mb), rows_mb)

    def wait_slices(buf, layer, lp, m, with_own):
        rows = rows_of(m)
        for d in ((0,) if with_own else ()) + (1, 3, 2):
            j = peer(d)
            ref = buf.at[layer, j, rows]
            pltpu.make_async_copy(ref, ref, ag_rsem.at[lp, j, m]).wait()

    def copy_out_slices(buf, out, layer, m, sem):
        rows = rows_of(m)
        for j in range(n_tp):
            pltpu.make_async_copy(buf.at[layer, j, rows], out.at[layer, rows, pl.ds(j * ds, ds)], sem).start()

    moved = lax.div(s, last)
    reducer = s + moved * (host_stage - last)

    def send_part(lp, d, m):
        rows = rows_of(m)
        pltpu.make_async_remote_copy(
            src_ref=rs_send.at[lp, d - 1, rows], dst_ref=rs_recv.at[moved, lp, d - 1, rows],
            send_sem=rs_ssem.at[lp], recv_sem=rs_rsem.at[moved, lp, d - 1, m],
            device_id={"pp": reducer, "tp": peer(d)}, device_id_type=pl.DeviceIdType.MESH).start()

    def send_slice(lp, buf, layer, lp_dst, stage, d, m):
        rows = rows_of(m)
        pltpu.make_async_remote_copy(
            src_ref=hs_send.at[lp, rows], dst_ref=buf.at[layer, t, rows],
            send_sem=ag_ssem.at[lp], recv_sem=ag_rsem.at[lp_dst, t, m],
            device_id={"pp": stage, "tp": peer(d)}, device_id_type=pl.DeviceIdType.MESH).start()

    def send_guest(lp, buf, layer, lp_dst, stage, m):
        rows = rows_of(m)
        for d in far_first + (0,):
            pltpu.make_async_remote_copy(
                src_ref=guest_send.at[lp, rows], dst_ref=buf.at[layer, t, rows],
                send_sem=guest_ssem.at[lp], recv_sem=ag_rsem.at[lp_dst, t, m],
                device_id={"pp": stage, "tp": peer(d)}, device_id_type=pl.DeviceIdType.MESH).start()

    def partials(lp, m, buf, layer, farthest, fn):
        rows = rows_of(m)
        for d in far_first:
            part = farthest if d == far_first[0] else fn(peer(d))
            rs_send[lp, d - 1, rows, :] = part.astype(BF16)
            send_part(lp, d, m)
        own = buf[layer, t, rows, :].astype(F32) + fn(t)

        @pl.when(s < away)
        def _():
            own_part[lp] = own

        @pl.when(s >= away)
        def _():
            own_send[lp, rows, :] = own
            pltpu.make_async_remote_copy(
                src_ref=own_send.at[lp, rows], dst_ref=guest_own.at[lp, rows],
                send_sem=own_ssem.at[lp], recv_sem=guest_rsem.at[lp, m],
                device_id={"pp": host_stage, "tp": t}, device_id_type=pl.DeviceIdType.MESH).start()

    def reduce_own(lp, m):
        rows = rows_of(m)
        for d in (1, 3, 2):
            ref = rs_recv.at[0, lp, d - 1, rows]
            pltpu.make_async_copy(ref, ref, rs_rsem.at[0, lp, d - 1, m]).wait()
        acc = own_part[lp]
        for d in (1, 3, 2):
            acc = acc + rs_recv[0, lp, d - 1, rows, :].astype(F32)
        return acc.astype(BF16)

    def reduce_guest(lp, m):
        rows = rows_of(m)
        for d in (1, 3, 2):
            ref = rs_recv.at[1, lp, d - 1, rows]
            pltpu.make_async_copy(ref, ref, rs_rsem.at[1, lp, d - 1, m]).wait()
        ref = guest_own.at[lp, rows]
        pltpu.make_async_copy(ref, ref, guest_rsem.at[lp, m]).wait()
        acc = guest_own[lp, rows, :]
        for d in (1, 3, 2):
            acc = acc + rs_recv[1, lp, d - 1, rows, :].astype(F32)
        return acc.astype(BF16)

    def fwd_a(layer, m):
        rows = rows_of(m)
        if layer == 0:
            @pl.when(s > 0)
            def _():
                wait_slices(a_buf, 0, 0, m, True)
        else:
            @pl.when(s < away)
            def _():
                wait_slices(a_buf, 1, 1, m, False)

            @pl.when(s >= away)
            def _():
                wait_slices(a_buf, 1, 1, m, True)
        for c in range(hidden // hc):
            cols = slice(c * hc, (c + 1) * hc)
            acc = dot(a_buf[layer, 0, rows, :], w1[layer, 0:ds, cols])
            for j in range(1, n_tp):
                acc = acc + dot(a_buf[layer, j, rows, :], w1[layer, j * ds:(j + 1) * ds, cols])
            u = acc.astype(BF16)
            g_buf[layer, rows, cols] = u
            z = gelu_fwd(u.astype(F32)).astype(BF16)
            z_buf[layer, rows, cols] = z
            part = dot(z, w2[layer, peer(far_first[0]), cols, :])
            farthest = part if c == 0 else farthest + part
        partials(layer, m, a_buf, layer, farthest, lambda j: dot(z_buf[layer, rows, :], w2[layer, j]))
        slope_buf[layer, rows, :] = gelu_grad(g_buf[layer, rows, :].astype(F32))
        copy_out_slices(a_buf, a_out, layer, m, out_sem.at[layer])
        pltpu.make_async_copy(z_buf.at[layer, rows], z_out.at[layer, rows], out_sem.at[4 + layer]).start()

    def fwd_b(layer, m):
        rows = rows_of(m)
        h = reduce_own(layer, m)
        hs_send[layer, rows, :] = h
        if layer == 0:
            for d in far_first:
                send_slice(0, a_buf, 1, 1, s, d, m)
            a_buf[1, t, rows, :] = h
        else:
            for d in far_first + (0,):
                send_slice(1, a_buf, 0, 0, s + 1, d, m)

    def fwd_b_guest(layer, m):
        rows = rows_of(m)
        h = reduce_guest(layer, m)
        if layer == 0:
            guest_send[0, rows, :] = h
            send_guest(0, a_buf, 1, 1, last, m)
            return
        err = h.astype(F32) - t_buf[rows, :].astype(F32)
        guest_send[1, rows, :] = (err * inv_count).astype(BF16)
        send_guest(1, dh_buf, 1, 3, last, m)
        half = 0.5 * err * err
        half = jnp.sum(half.reshape(rows_mb // 8, 8, ds), axis=0)
        part = half[:, :128]
        for q in range(1, ds // 128):
            part = part + half[:, q * 128:(q + 1) * 128]
        loss_acc[...] = loss_acc[...] + part

        @pl.when(m == n_mb - 1)
        def _():
            for d in far_first + (0,):
                pltpu.make_async_remote_copy(
                    src_ref=loss_acc, dst_ref=loss_all.at[t],
                    send_sem=loss_ssem.at[0], recv_sem=lall_rsem.at[t],
                    device_id={"pp": last, "tp": peer(d)}, device_id_type=pl.DeviceIdType.MESH).start()

    def pass_loss():
        @pl.when(s == last)
        def _():
            for j in range(n_tp):
                pltpu.make_async_copy(loss_all.at[j], loss_all.at[j], lall_rsem.at[j]).wait()
            tot = loss_all[0]
            for j in range(1, n_tp):
                tot = tot + loss_all[j]
            loss_tot[...] = tot

        @pl.when(s < last)
        def _():
            pltpu.make_async_copy(loss_tot, loss_tot, ltot_rsem).wait()

        @pl.when(s > 0)
        def _():
            pltpu.make_async_remote_copy(
                src_ref=loss_tot, dst_ref=loss_tot, send_sem=loss_ssem.at[1], recv_sem=ltot_rsem,
                device_id={"pp": s - 1, "tp": t}, device_id_type=pl.DeviceIdType.MESH).start()

    def bwd_a(layer, m):
        lp = 2 + layer
        rows = rows_of(m)
        if layer == 1:
            wait_slices(dh_buf, 1, 3, m, True)
        else:
            @pl.when(s < away)
            def _():
                wait_slices(dh_buf, 0, 2, m, False)

            @pl.when(s >= away)
            def _():
                wait_slices(dh_buf, 0, 2, m, True)
        far_rows = pl.ds(pl.multiple_of(peer(far_first[0]) * ds, ds), ds)
        for c in range(hidden // hc):
            cols = slice(c * hc, (c + 1) * hc)
            acc = dot_t(dh_buf[layer, 0, rows, :], w2[layer, 0, cols, :])
            for j in range(1, n_tp):
                acc = acc + dot_t(dh_buf[layer, j, rows, :], w2[layer, j, cols, :])
            g = (slope_buf[layer, rows, cols] * acc).astype(BF16)
            g_buf[layer, rows, cols] = g
            part = dot_t(g, w1[layer, far_rows, cols])
            farthest = part if c == 0 else farthest + part

        def send():
            partials(lp, m, dh_buf, layer, farthest, lambda j: dot_t(
                g_buf[layer, rows, :], w1[layer, pl.ds(pl.multiple_of(j * ds, ds), ds), :]))

        if layer == 1:
            send()
        else:
            pl.when(s > 0)(send)
        copy_out_slices(dh_buf, dh_out, layer, m, out_sem.at[2 + layer])
        pltpu.make_async_copy(g_buf.at[layer, rows], g_out.at[layer, rows], out_sem.at[6 + layer]).start()
        if layer == 1:
            pl.when(m == n_mb - 1)(pass_loss)

    def bwd_b(layer, m):
        lp = 2 + layer
        rows = rows_of(m)
        h = reduce_own(lp, m)
        hs_send[lp, rows, :] = h
        if layer == 1:
            for d in far_first:
                send_slice(lp, dh_buf, 0, 2, s, d, m)
            dh_buf[0, t, rows, :] = h
        else:
            for d in far_first + (0,):
                send_slice(lp, dh_buf, 1, 3, s - 1, d, m)

    def bwd_b_guest(layer, m):
        lp = 2 + layer
        rows = rows_of(m)
        guest_send[lp, rows, :] = reduce_guest(lp, m)
        if layer == 1:
            send_guest(lp, dh_buf, 0, 2, last, m)
        else:
            send_guest(lp, dh_buf, 1, 3, last - 1, m)

    f_start = 4 * s
    b_start = 2 * n_layer + shift + 4 * (last - s)

    def tick(k, carry):
        @pl.when(k == 1)
        def _():
            for c in loads[1]:
                c.wait()

        @pl.when((k == 1) & (s == 0))
        def _():
            for c in x_tail:
                c.wait()

        @pl.when((k == 1) & (s == host_stage))
        def _():
            y_load.wait()

        bias = 8 * n_pp + 2 * n_layer + shift + 4 + spacing
        bias = spacing * (-(-bias // spacing))
        turn = {}
        for name, start in (("f", f_start), ("b", b_start)):
            q = k - start + bias
            turn[name] = (lax.div(q, spacing) - bias // spacing, lax.rem(q, spacing) if spacing > 1 else None)

        def at(name, offset, fn, layer, extra=None):
            m, phase = turn[name]
            m = m - offset // spacing
            ok = (m >= 0) & (m < n_mb)
            if phase is not None:
                ok = ok & (phase == offset % spacing)
            if extra is not None:
                ok = ok & extra
            pl.when(ok)(lambda: fn(layer, m))

        here, host, far = s < away, s == host_stage, 4 * (last - host_stage)
        at("b", 3, bwd_b, 0, here & (s > 0))
        at("b", 3 - far, bwd_b_guest, 0, host)
        at("b", 2, bwd_a, 0)
        at("b", 1, bwd_b, 1, here)
        at("b", 1 - far, bwd_b_guest, 1, host)
        at("b", 0, bwd_a, 1)
        at("f", 3, fwd_b, 1, here)
        at("f", 3 + far, fwd_b_guest, 1, host)
        at("f", 2, fwd_a, 1)
        at("f", 1, fwd_b, 0, here)
        at("f", 1 + far, fwd_b_guest, 0, host)
        at("f", 0, fwd_a, 0)
        return carry

    n_ticks = 4 * n_layer + shift + spacing * (n_mb - 1)
    lax.fori_loop(0, n_ticks, tick, 0)

    for layer in range(2):
        for i in range(4):
            pltpu.make_async_copy(z_buf.at[layer], z_out.at[layer], out_sem.at[2 * i + layer]).wait()

    def wait_three(sem):
        pltpu.make_async_copy(rs_send.at[0], rs_send.at[0], sem).wait()

    def wait_four(sem):
        pltpu.make_async_copy(a_buf.at[0], a_buf.at[0], sem).wait()

    for lp in (0, 1, 3):
        wait_three(rs_ssem.at[lp])

    @pl.when(s < away)
    def _():
        wait_three(ag_ssem.at[0])
        wait_three(ag_ssem.at[3])
        wait_four(ag_ssem.at[1])

    @pl.when((s < away) & (s > 0))
    def _():
        wait_four(ag_ssem.at[2])

    @pl.when(s >= away)
    def _():
        for lp in range(4):
            pltpu.make_async_copy(own_send.at[lp], own_send.at[lp], own_ssem.at[lp]).wait()

    @pl.when(s == host_stage)
    def _():
        for lp in range(4):
            wait_four(guest_ssem.at[lp])

    @pl.when(s == host_stage)
    def _():
        pltpu.make_async_copy(loss_all, loss_all, loss_ssem.at[0]).wait()

    @pl.when(s > 0)
    def _():
        wait_three(rs_ssem.at[2])
        pltpu.make_async_copy(loss_tot, loss_tot, loss_ssem.at[1]).wait()

    loss_out[...] = loss_tot[...]


def dot_tokens(a, b):
    return lax.dot_general(a, b, (((0,), (0,)), ((), ())), preferred_element_type=F32)


def grad_kernel(inv_count, a_ref, g_ref, z_ref, dh_ref, loss_ref, first_ref, second_ref, total_ref):
    @pl.when((pl.program_id(0) == 0) & (pl.program_id(1) == 0))
    def _():
        total_ref[0, 0] = jnp.sum(loss_ref[...]) * inv_count

    first_ref[0] = dot_tokens(a_ref[0], g_ref[0])
    second_ref[0] = dot_tokens(z_ref[0], dh_ref[0])


def weight_grads(a, g, z, dh, loss, inv_count):
    n_layer, n_tok, d_model = a.shape
    hidden = g.shape[2]
    steps = d_model // GRAD_TILE
    rows2 = hidden // steps
    return pl.pallas_call(
        functools.partial(grad_kernel, inv_count),
        grid=(n_layer, steps),
        in_specs=[
            pl.BlockSpec((1, n_tok, GRAD_TILE), lambda l, j: (l, 0, j)),
            pl.BlockSpec((1, n_tok, hidden), lambda l, j: (l, 0, 0)),
            pl.BlockSpec((1, n_tok, rows2), lambda l, j: (l, 0, j)),
            pl.BlockSpec((1, n_tok, d_model), lambda l, j: (l, 0, 0)),
            pl.BlockSpec((8, 128), lambda l, j: (0, 0)),
        ],
        out_specs=[
            pl.BlockSpec((1, GRAD_TILE, hidden), lambda l, j: (l, j, 0)),
            pl.BlockSpec((1, rows2, d_model), lambda l, j: (l, j, 0)),
            pl.BlockSpec(memory_space=pltpu.SMEM),
        ],
        out_shape=[
            jax.ShapeDtypeStruct((n_layer, d_model, hidden), F32),
            jax.ShapeDtypeStruct((n_layer, hidden, d_model), F32),
            jax.ShapeDtypeStruct((1, 1), F32),
        ],
        compiler_params=pltpu.CompilerParams(vmem_limit_bytes=63 * 1024 * 1024),
        cost_estimate=pl.CostEstimate(
            flops=8 * n_tok * d_model * hidden, bytes_accessed=4 * n_layer * 2 * n_tok * d_model * 2, transcendentals=0),
        name="weight_grads",
    )(a, g, z, dh, loss)


def solution(mesh):
    n_pp = mesh.shape["pp"]
    n_tp = mesh.shape["tp"]

    def device_program(x_loc, y_loc, w_in, w_out):
        n_tok = x_loc.shape[0] * x_loc.shape[1]
        d_model = x_loc.shape[2]
        hidden = w_in.shape[3]
        ds = d_model // n_tp
        rows_mb = CHUNK
        n_mb = n_tok // rows_mb
        inv_count = 1.0 / (n_tok * d_model)
        kernel = functools.partial(stack_kernel, n_pp, n_tp, rows_mb, SPACING, SHIFT, inv_count)
        any_spec = pl.BlockSpec(memory_space=pl.ANY)
        dma = pltpu.SemaphoreType.DMA
        a, dh, z, g, loss = pl.pallas_call(
            kernel,
            out_shape=[
                jax.ShapeDtypeStruct((2, n_tok, d_model), BF16),
                jax.ShapeDtypeStruct((2, n_tok, d_model), BF16),
                jax.ShapeDtypeStruct((2, n_tok, hidden), BF16),
                jax.ShapeDtypeStruct((2, n_tok, hidden), BF16),
                jax.ShapeDtypeStruct((8, 128), F32),
            ],
            in_specs=[any_spec] * 4,
            out_specs=[any_spec] * 4 + [pl.BlockSpec(memory_space=pltpu.VMEM)],
            scratch_shapes=[
                pltpu.VMEM((2, d_model, hidden), BF16),
                pltpu.VMEM((2, n_tp, hidden, ds), BF16),
                pltpu.VMEM((2, n_tp, n_tok, ds), BF16),
                pltpu.VMEM((2, n_tp, n_tok, ds), BF16),
                pltpu.VMEM((2, n_tok, hidden), F32),
                pltpu.VMEM((2, n_tok, hidden), BF16),
                pltpu.VMEM((2, n_tok, hidden), BF16),
                pltpu.VMEM((2, 4, 3, n_tok, ds), BF16),
                pltpu.VMEM((4, 3, n_tok, ds), BF16),
                pltpu.VMEM((4, n_tok, ds), BF16),
                pltpu.VMEM((4, rows_mb, ds), F32),
                pltpu.VMEM((n_tok, ds), BF16),
                pltpu.VMEM((8, 128), F32),
                pltpu.VMEM((n_tp, 8, 128), F32),
                pltpu.VMEM((8, 128), F32),
                pltpu.VMEM((4, n_tok, ds), F32),
                pltpu.VMEM((4, n_tok, ds), F32),
                pltpu.VMEM((4, n_tok, ds), BF16),
                dma((3 + 4 * n_tp,)),
                dma((2, 4, 3, n_mb)),
                dma((4, n_tp, n_mb)),
                dma((4,)),
                dma((4,)),
                dma((8,)),
                dma((4, n_mb)),
                dma((4,)),
                dma((4,)),
                dma((n_tp,)),
                dma,
                dma((2,)),
            ],
            compiler_params=pltpu.CompilerParams(has_side_effects=True, vmem_limit_bytes=67043328),
            cost_estimate=pl.CostEstimate(flops=10**11, bytes_accessed=10**8, transcendentals=0),
            name="mlp_stack",
        )(x_loc.reshape(n_tok, d_model), y_loc.reshape(n_tok, d_model), w_in[0], w_out[0])
        grad_first, grad_second, loss_val = weight_grads(a, g, z, dh, loss, inv_count)
        grad_first, grad_second = grad_first[None], grad_second[None]
        return grad_first, grad_second, loss_val.reshape(1)

    return jax.shard_map(
        device_program,
        mesh=mesh,
        in_specs=(P("dp", None, None), P("dp", None, None), P("pp", None, None, "tp"), P("pp", None, "tp", None)),
        out_specs=(P(("dp", "pp"), None, None, "tp"), P(("dp", "pp"), None, "tp", None), P("dp")),
        check_vma=False,
    )
```
